512 devices in a mesh: tm: 4 (over y), row: 16 (over z), col: 8 (over x, core).
Axes of the slice: x: 4, y: 4, z: 16, core: 2. Of those that a mesh axis runs over, the one named last changes fastest.
Arguments:
- noisy_video: float32 [16, 2048, 2048], P('tm', 'row', 'col'), may hold values from -6 to 6
- fidelity: float32 [16, 2048, 2048], P('tm', 'row', 'col'), may hold values from 0.5 to 12, as said below
Outputs:
- denoised: float32 [16, 2048, 2048], P('tm', 'row', 'col')
- gaps: float32 [3], replicated
The draws below stay inside these ranges and needn't reach their ends.
Inputs may be any that keep to these rules, and one draw needn't show every extreme that they name: `fidelity`: positive, larger on average toward later rows.
All inputs are finite; a program needn't handle non-finite values.
Results may differ from the reference program's by a relative error of at most 0.0001.
Values sent between devices are 32-bit elements; how exact they have to be, the bound alone decides.
No kernel may reach another device: no remote copies, remote signals or barrier semaphores. Data moves between devices by JAX's collectives and lax.ppermute only.
A program may use at most 64 MiB of HBM per device.

```python
import math
import jax
import jax.numpy as jnp
from jax import lax

ITERS = 3
NT = 16
NH = 2048
NW = 2048


def draw_fidelity(key, part):
    inner = jax.random.fold_in(key, 11)
    base = jnp.exp(jax.random.uniform(inner, (NT, NH, NW), jnp.float32, math.log(0.5), math.log(4.0)))
    ramp = jnp.power(3.0, jnp.arange(NH, dtype=jnp.float32) / float(NH))
    return (base * ramp[None, :, None]).astype(jnp.float32)


def shard_levels(stream_key, dims, split, smallest, top_value):
    def one(dim, shards_of):
        steps = jax.random.uniform(jax.random.fold_in(jax.random.fold_in(stream_key, 6), dim), (shards_of,), jnp.float32, smallest / len(split), top_value / len(split))
        return jnp.repeat(jnp.exp(steps), dims[dim] // shards_of).reshape((-1,) + (1,) * (len(dims) - dim - 1))

    loudness = one(*split[0])
    for cut in split[1:]:
        loudness = loudness * one(*cut)
    return loudness


def normal_values(rng, dims, width, bound, cuts=(), kind=jnp.bfloat16):
    factor_of = shard_levels(rng, dims, cuts, -0.22, 0.18) if cuts else 1.0
    drawn = jax.random.normal(rng, dims, jnp.float32) * width * factor_of
    return jnp.minimum(jnp.maximum(drawn, -bound), bound).astype(kind)


def setup_inputs(seed: int = 0) -> dict:
    splits = jax.random.split(jax.random.key(seed), 3)
    noisy_video = normal_values(splits[0], (NT, NH, NW), 1.0, 6.0, ((0, 4), (1, 16), (2, 8)), jnp.float32)
    fidelity = draw_fidelity(jax.random.fold_in(splits[2], 71), 0)
    return dict(noisy_video=noisy_video, fidelity=fidelity)


sigma_step = 0.28
tau_step = 0.28

def forward(field, axis):
    count = field.shape[axis]
    ahead = lax.slice_in_dim(field, 1, count, axis=axis) - lax.slice_in_dim(field, 0, count - 1, axis=axis)
    edge = jnp.zeros_like(lax.slice_in_dim(field, 0, 1, axis=axis))
    return jnp.concatenate([ahead, edge], axis=axis)

def backward(comp, axis):
    count = comp.shape[axis]
    edge = jnp.zeros_like(lax.slice_in_dim(comp, 0, 1, axis=axis))
    before = jnp.concatenate([edge, lax.slice_in_dim(comp, 0, count - 1, axis=axis)], axis=axis)
    return comp - before

def reference(noisy_video, fidelity):
    field = noisy_video
    ubar_field = noisy_video
    zero_field = jnp.zeros_like(noisy_video)
    duals = [zero_field, zero_field, zero_field]
    grad_u = None
    gap_list = []
    for iteration in range(ITERS):
        grads = [forward(ubar_field, 0), forward(ubar_field, 1), forward(ubar_field, 2)]
        if iteration == 0:
            grad_u = grads
        else:
            grad_u = [0.5 * (grads[0] + grad_u[0]), 0.5 * (grads[1] + grad_u[1]), 0.5 * (grads[2] + grad_u[2])]
        moved = [duals[0] + sigma_step * grads[0], duals[1] + sigma_step * grads[1], duals[2] + sigma_step * grads[2]]
        length = jnp.sqrt(moved[0] * moved[0] + moved[1] * moved[1] + moved[2] * moved[2])
        scale = jnp.maximum(1.0, length)
        duals = [moved[0] / scale, moved[1] / scale, moved[2] / scale]
        diverge = backward(duals[0], 0) + backward(duals[1], 1) + backward(duals[2], 2)
        total_var = jnp.sqrt(grad_u[0] * grad_u[0] + grad_u[1] * grad_u[1] + grad_u[2] * grad_u[2])
        resid = field - noisy_video
        term = 0.5 * fidelity * resid * resid + total_var + diverge * diverge / (2.0 * fidelity) + noisy_video * diverge
        gap_list.append(jnp.sum(term) / float(term.size))
        new_field = (field + tau_step * diverge + tau_step * fidelity * noisy_video) / (1.0 + tau_step * fidelity)
        ubar_field = 2.0 * new_field - field
        field = new_field
    return (field, jnp.stack(gap_list).astype(jnp.float32))
```

```python
import functools

import jax
import jax.numpy as jnp
from jax import lax
from jax.experimental import pallas as pl
from jax.experimental.pallas import tpu as pltpu
from jax.sharding import PartitionSpec as P

SIG = 0.28
TAU = 0.28

FR = 4
NT = 16
NTE = 17
NF = 10
NL = 8
LW = 3
LOFF = 64


def iota(axis):
    return lax.broadcasted_iota(jnp.int32, (8, 128), axis)


def tile(ref, lead, i, j):
    return ref[lead, i * 8 : (i + 1) * 8, j * 128 : (j + 1) * 128]


def put(ref, lead, i, j, value):
    ref[lead, i * 8 : (i + 1) * 8, j * 128 : (j + 1) * 128] = value


def lanes_of(lane, planes):
    hit = None
    for p in planes:
        for base in (0, LOFF):
            here = (lane >= base + LW * p) & (lane < base + LW * p + LW)
            hit = here if hit is None else hit | here
    return hit


def pack_kernel(f_ref, l_ref, s_ref, up_ref, dn_ref):
    sub, lane = iota(0), iota(1)
    for i in range(NT):
        acc = jnp.zeros((8, 128), jnp.float32)
        for t in range(FR):
            for ref, p in ((f_ref, t + 3), (l_ref, t + 12)):
                right = pltpu.roll(tile(ref, t, i, 1), (LW * p - 125) % 128, 1)
                left = pltpu.roll(tile(ref, t, i, 0), (LOFF + LW * p) % 128, 1)
                acc = jnp.where((lane >= LW * p) & (lane < LW * p + LW), right, acc)
                acc = jnp.where((lane >= LOFF + LW * p) & (lane < LOFF + LW * p + LW), left, acc)
        s_ref[i] = acc
    for t in range(FR):
        for k, ref in ((0, f_ref), (4, l_ref)):
            for j in range(2):
                s_ref[NT + 2 * (t + k) + j] = jnp.where(sub < 4, tile(ref, t, 0, j), tile(ref, t, NT - 1, j))
    up_ref[0:3] = f_ref[1:4]
    up_ref[3:5] = l_ref[2:4]
    dn_ref[0:3] = f_ref[0:3]
    dn_ref[3:5] = l_ref[0:2]


def rows_kernel(own_ref, prev_ref, next_ref, z_ref):
    def move(src, plane, dst):
        for j in range(2):
            z_ref[2 * dst + j] = src[NT + 2 * plane + j]

    for k in range(3):
        move(prev_ref, k + 1, k)
        move(next_ref, k, 7 + k)
    for k in range(4):
        move(own_ref, k, 3 + k)
        move(own_ref, 4 + k, 12 + k)
    for k in range(2):
        move(prev_ref, 6 + k, 10 + k)
        move(next_ref, 4 + k, 16 + k)


def cols_kernel(own_ref, prev_ref, next_ref, zp_ref, zn_ref, m_ref):
    sub, lane = iota(0), iota(1)
    from_prev = lanes_of(lane, (0, 1, 2, 10, 11))
    from_next = lanes_of(lane, (7, 8, 9, 16, 17))
    for i in range(NT):
        a = pltpu.roll(prev_ref[i], 128 - 12, 1)
        b = pltpu.roll(next_ref[i], 12, 1)
        m_ref[i] = jnp.where(from_prev, a, jnp.where(from_next, b, own_ref[i]))
    acc = jnp.zeros((8, 128), jnp.float32)
    for p in range(NF + NL):
        left = jnp.where(sub < 4, zn_ref[2 * p], zp_ref[2 * p])
        right = jnp.where(sub < 4, zn_ref[2 * p + 1], zp_ref[2 * p + 1])
        right = pltpu.roll(right, (LW * p - 125) % 128, 1)
        left = pltpu.roll(left, (LOFF + LW * p) % 128, 1)
        acc = jnp.where((lane >= LW * p) & (lane < LW * p + LW), right, acc)
        acc = jnp.where((lane >= LOFF + LW * p) & (lane < LOFF + LW * p + LW), left, acc)
    m_ref[NT] = acc


def main_kernel(
    sizes, f_ref, l_ref, bp_ref, bn_ref, zp_ref, zn_ref, mp_ref, mn_ref,
    out_ref, sum_ref,
    ua, ub, qa, qb, v1, v2, wt, at, il, g1, g2,
):
    n_tm, n_row, n_col = sizes
    sub, lane = iota(0), iota(1)
    first_t = lax.axis_index("tm") == 0
    last_t = lax.axis_index("tm") == n_tm - 1
    one, zero = jnp.float32(1.0), jnp.float32(0.0)
    last_r = jnp.where(lax.axis_index("row") == n_row - 1, zero, one)
    first_r = jnp.where(lax.axis_index("row") == 0, zero, one)
    last_c = jnp.where(lax.axis_index("col") == n_col - 1, zero, one)
    first_c = jnp.where(lax.axis_index("col") == 0, zero, one)
    ones = jnp.ones((8, 128), jnp.float32)
    row_mask = {NT - 1: jnp.where(sub == 7, ones * last_r, ones), NT: jnp.where(sub == 7, ones * first_r, ones)}
    col_mask = {1: jnp.where(lane == 127, ones * last_c, ones), 2: jnp.where(lane == 127, ones * first_c, ones)}

    def prim(lam, noisy):
        scaled = TAU * lam
        return 1.0 / (1.0 + scaled), scaled * noisy

    def fill_noisy(src, at0, dst):
        for i in range(NT):
            for j in range(2):
                put(ua, dst, i, j, tile(src, at0, i, j))

    def fill_lam(src, at0, dst):
        for i in range(NT):
            for j in range(2):
                w, a = prim(tile(src, at0, i, j), tile(ua, dst + 1, i, j))
                put(wt, dst, i, j, w)
                put(at, dst, i, j, a)

    def own(t, c):
        fill_noisy(f_ref, t, t + 3)
        for i in range(NT):
            for j in range(2):
                lam = tile(l_ref, t, i, j)
                w, a = prim(lam, tile(f_ref, t, i, j))
                put(wt, t + 2, i, j, w)
                put(at, t + 2, i, j, a)
                put(il, t, i, j, 0.5 / lam)
        return c

    lax.fori_loop(0, FR, own, 0)

    def face(k, c):
        fill_noisy(bp_ref, k, k)
        fill_noisy(bn_ref, k, k + 7)
        return c

    lax.fori_loop(0, 3, face, 0)

    def face_lam(k, c):
        fill_lam(bp_ref, 3 + k, k)
        fill_lam(bn_ref, 3 + k, 6 + k)
        return c

    lax.fori_loop(0, 2, face_lam, 0)
    for p in range(NF + NL):
        for j in range(2):
            z = jnp.where(sub < 4, zn_ref[2 * p + j], zp_ref[2 * p + j])
            if p < NF:
                put(ua, p, NT, j, z)
            else:
                w, a = prim(z, tile(ua, p - NF + 1, NT, j))
                put(wt, p - NF, NT, j, w)
                put(at, p - NF, NT, j, a)

    def side(i, c):
        rows = pl.ds(pl.multiple_of(i * 8, 8), 8)
        mp, mn = mp_ref[i], mn_ref[i]
        noisy = []
        for p in range(NF + NL):
            right = pltpu.roll(mn, (-(LOFF + LW * p)) % 128, 1)
            left = pltpu.roll(mp, (125 - LW * p) % 128, 1)
            x = jnp.where(lane < 3, right, jnp.where(lane >= 125, left, 0.0))
            if p < NF:
                ua[p, rows, 256:384] = x
                noisy.append(x)
            else:
                w, a = prim(x, noisy[p - NF + 1])
                wt[p - NF, rows, 256:384] = w
                at[p - NF, rows, 256:384] = a
        return c

    lax.fori_loop(0, NTE, side, 0)

    def dual_step(step, u, qi, qo, tt, gi, go, acc):
        inside = acc is not None
        keep = jnp.where(((tt == 6) & last_t) | ((tt == 2) & first_t), zero, one)
        here = [tile(u, tt, 0, j) for j in range(3)]
        start = here
        for i in range(NTE):
            after = start if i == NT else [tile(u, tt, i + 1, j) for j in range(3)]
            turned = [pltpu.roll(here[j], 127, 1) for j in range(3)]
            for j in range(3):
                x = here[j]
                d0 = (tile(u, tt + 1, i, j) - x) * keep
                d1 = pltpu.roll(jnp.where(sub == 0, after[j], x), 7, 0) - x
                if i in row_mask:
                    d1 = d1 * row_mask[i]
                d2 = jnp.where(lane == 127, turned[(j + 1) % 3], turned[j]) - x
                if j in col_mask:
                    d2 = d2 * col_mask[j]
                d = (d0, d1, d2)
                if inside and i < NT and j < 2:
                    gu = d
                    t = tt - 3
                    if step > 0:
                        gu = tuple(0.5 * (d[k] + tile(gi, 4 * k + t, i, j)) for k in range(3))
                    if step < 2:
                        for k in range(3):
                            put(go, 4 * k + t, i, j, gu[k])
                    acc[j] = acc[j] + jnp.sqrt(gu[0] * gu[0] + gu[1] * gu[1] + gu[2] * gu[2])
                m = d if step == 0 else tuple(d[k] + tile(qi, NF * k + tt, i, j) for k in range(3))
                n2 = (m[0] * m[0] + m[1] * m[1] + m[2] * m[2]) * (SIG * SIG)
                s = jnp.minimum(1.0, lax.rsqrt(n2))
                for k in range(3):
                    put(qo, NF * k + tt, i, j, m[k] * s)
            here = after

    def primal_step(step, u, q, vi, vo, uo, tt, acc):
        inside = acc is not None
        nj = 3 if step < 2 else 2
        before = [tile(q, NF + tt, NT, j) for j in range(nj)]
        for i in range(NTE if step < 2 else NT):
            rows = [tile(q, NF + tt, i, j) for j in range(nj)]
            cols = [tile(q, 2 * NF + tt, i, j) for j in range(3)]
            turned = [pltpu.roll(cols[j], 1, 1) for j in range(3)]
            for j in range(nj):
                d = tile(q, tt, i, j) - tile(q, tt - 1, i, j)
                d = d + (rows[j] - pltpu.roll(jnp.where(sub == 7, before[j], rows[j]), 1, 0))
                d = d + (cols[j] - jnp.where(lane == 0, turned[j - 1], turned[j]))
                old = tile(u, tt, i, j) if step == 0 else tile(vi, tt, i, j)
                new = (old + (TAU * SIG) * d + tile(at, tt - 1, i, j)) * tile(wt, tt - 1, i, j)
                if step < 2:
                    put(vo, tt, i, j, new)
                    put(uo, tt, i, j, 2.0 * new - old)
                else:
                    put(out_ref, tt - 3, i, j, new)
                if inside and i < NT and j < 2:
                    t = tt - 3
                    e = SIG * d
                    noisy = tile(f_ref, t, i, j)
                    term = e * (e * tile(il, t, i, j) + noisy)
                    if step > 0:
                        r = old - noisy
                        term = term + (0.5 * tile(l_ref, t, i, j)) * (r * r)
                    acc[j] = acc[j] + term
            before = rows

    def run(step, u, uo, qi, qo, vi, vo, gi, go):
        lo, hi = step, 8 - step

        def dual_out(k, c):
            dual_step(step, u, qi, qo, jnp.where(k < 3, k, k + 4), gi, go, None)
            return c

        def dual_in(tt, c):
            acc = list(c)
            dual_step(step, u, qi, qo, tt, gi, go, acc)
            return tuple(acc)

        def primal_out(k, c):
            primal_step(step, u, qo, vi, vo, uo, jnp.where(k < 3, k, k + 4), None)
            return c

        def primal_in(tt, c):
            acc = list(c)
            primal_step(step, u, qo, vi, vo, uo, tt, acc)
            return tuple(acc)

        blank = jnp.zeros((8, 128), jnp.float32)
        lax.fori_loop(lo, hi - 3, dual_out, 0)
        acc = lax.fori_loop(3, 7, dual_in, (blank, blank))
        if step < 2:
            lax.fori_loop(lo + 1, hi - 3, primal_out, 0)
        acc = lax.fori_loop(3, 7, primal_in, acc)
        return acc[0] + acc[1]

    s0 = run(0, ua, ub, qb, qa, None, v1, None, g1)
    s1 = run(1, ub, ua, qa, qb, v1, v2, g1, g2)
    s2 = run(2, ua, None, qb, qa, v2, None, g2, None)
    total = [jnp.sum(s) for s in (s0, s1, s2)]
    col = lax.broadcasted_iota(jnp.int32, sum_ref.shape, 1)
    sum_ref[...] = jnp.where(col == 0, total[0], jnp.where(col == 1, total[1], jnp.where(col == 2, total[2], 0.0)))


VMEM = pl.BlockSpec(memory_space=pltpu.VMEM)


def call(kernel, outs, *args, flops, scratch=(), limit=None):
    return pl.pallas_call(
        kernel,
        out_shape=outs,
        in_specs=[VMEM] * len(args),
        out_specs=jax.tree.map(lambda _: VMEM, outs),
        scratch_shapes=scratch,
        cost_estimate=pl.CostEstimate(flops=flops, bytes_accessed=1 << 20, transcendentals=0),
        compiler_params=pltpu.CompilerParams(vmem_limit_bytes=limit),
    )(*args)


def f32(*shape):
    return jax.ShapeDtypeStruct(shape, jnp.float32)


def both_ways(later, earlier, axis):
    n = lax.axis_size(axis)
    onward = lax.ppermute(later, axis, [(i, i + 1) for i in range(n - 1)])
    back = lax.ppermute(earlier, axis, [(i + 1, i) for i in range(n - 1)])
    return onward, back


def on_device(noisy, lam):
    n_tm, n_row, n_col = (lax.axis_size(a) for a in ("tm", "row", "col"))
    cells = float(noisy.size * n_tm * n_row * n_col)
    strip, up, down = call(
        pack_kernel, (f32(NT + 16, 8, 128), f32(5, 128, 256), f32(5, 128, 256)), noisy, lam, flops=1 << 20
    )
    sp, sn = both_ways(strip, strip, "tm")
    up, down, _, _ = lax.optimization_barrier((up, down, strip, strip))
    bp, bn = both_ways(up, down, "tm")
    z = call(rows_kernel, f32(2 * (NF + NL), 8, 128), strip, sp, sn, flops=1 << 20)
    zp, zn = both_ways(z, z, "row")
    m = call(cols_kernel, f32(NTE, 8, 128), strip, sp, sn, zp, zn, flops=1 << 20)
    mp, mn = both_ways(m, m, "col")
    ext = lambda n: pltpu.VMEM((n, NTE * 8, 384), jnp.float32)
    inner = lambda n: pltpu.VMEM((n, 128, 256), jnp.float32)
    out, rows = call(
        functools.partial(main_kernel, (n_tm, n_row, n_col)),
        (f32(4, 128, 256), f32(n_row, 128)),
        noisy, lam, bp, bn, zp, zn, mp, mn,
        flops=1 << 26,
        scratch=[ext(NF), ext(NF), ext(3 * NF), ext(3 * NF), ext(NF), ext(NF), ext(NL), ext(NL), inner(4), inner(12), inner(12)],
        limit=40 << 20,
    )
    part = jnp.sum(lax.all_to_all(rows, "row", 0, 0, tiled=True), 0, keepdims=True)
    part = jnp.broadcast_to(part, (n_tm * n_col, 128))
    part = jnp.sum(lax.all_to_all(part, ("tm", "col"), 0, 0, tiled=True), 0)
    gaps = part[:3] / cells
    return out, gaps


def solution(mesh):
    spec = P("tm", "row", "col")
    return jax.shard_map(on_device, mesh=mesh, in_specs=(spec, spec), out_specs=(spec, P()), check_vma=False)
```

```python
import functools

import jax
import jax.numpy as jnp
from jax import lax
from jax.experimental import pallas as pl
from jax.experimental.pallas import tpu as pltpu
from jax.sharding import PartitionSpec as P


SIG = 0.28
TAU = 0.28

FR = 4
NT = 16
NTE = 17
NF = 10
NL = 8
NP = NF + NL
LW = 6


def iota(axis):
    return lax.broadcasted_iota(jnp.int32, (8, 128), axis)


def tile(ref, lead, i, j):
    return ref[lead, i * 8 : (i + 1) * 8, j * 128 : (j + 1) * 128]


def put(ref, lead, i, j, value):
    ref[lead, i * 8 : (i + 1) * 8, j * 128 : (j + 1) * 128] = value


def lanes_of(lane, planes):
    hit = None
    for p in planes:
        here = (lane >= LW * p) & (lane < LW * p + LW)
        hit = here if hit is None else hit | here
    return hit


def strip_of(lane, acc, p, first, last):
    both = pltpu.roll(jnp.where(lane < 64, first, last), (LW * p - 125) % 128, 1)
    return jnp.where((lane >= LW * p) & (lane < LW * p + LW), both, acc)


def pack_kernel(f_hbm, l_hbm, own_ref, z_ref, on_ref, back_ref, up_ref, dn_ref, fv, lv, sems):
    sub, lane = iota(0), iota(1)
    copies = []
    for t in range(FR):
        for k, (src, dst) in enumerate(((f_hbm, fv), (l_hbm, lv))):
            copies.append(pltpu.make_async_copy(src.at[t], dst.at[t], sems.at[2 * t + k]))
            copies[-1].start()
    for copy in copies:
        copy.wait()
    for i in range(NT):
        acc = jnp.zeros((8, 128), jnp.float32)
        for t in range(FR):
            acc = strip_of(lane, acc, t + 3, tile(fv, t, i, 0), tile(fv, t, i, 1))
            acc = strip_of(lane, acc, t + 12, tile(lv, t, i, 0), tile(lv, t, i, 1))
        own_ref[i] = acc
        on_ref[i] = acc
        back_ref[i] = acc
    for t in range(FR):
        for k, ref in ((0, fv), (1, lv)):
            for j in range(2):
                z = jnp.where(sub < 4, tile(ref, t, 0, j), tile(ref, t, NT - 1, j))
                z_ref[2 * (t + 4 * k) + j] = z
                o = t - 1 if k == 0 else t + 1
                if (k == 0 and t >= 1) or (k == 1 and t >= 2):
                    on_ref[NT + 2 * o + j] = z
                o = t if k == 0 else t + 3
                if (k == 0 and t < 3) or (k == 1 and t < 2):
                    back_ref[NT + 2 * o + j] = z
    up_ref[0:3] = fv[1:4]
    up_ref[3:5] = lv[2:4]
    dn_ref[0:3] = fv[0:3]
    dn_ref[3:5] = lv[0:2]


def rows_kernel(z_ref, prev_ref, next_ref, on_ref, back_ref):
    sub = iota(0)

    def plane(p, j):
        if p < 3:
            return prev_ref[NT + 2 * p + j]
        if p < 7:
            return z_ref[2 * (p - 3) + j]
        if p < 10:
            return next_ref[NT + 2 * (p - 7) + j]
        if p < 12:
            return prev_ref[NT + 2 * (p - 7) + j]
        if p < 16:
            return z_ref[2 * (p - 8) + j]
        return next_ref[NT + 2 * (p - 13) + j]

    for m in range(NP // 2):
        for j in range(2):
            a, b = plane(2 * m, j), pltpu.roll(plane(2 * m + 1, j), 4, 0)
            on_ref[2 * m + j] = jnp.where(sub < 4, b, a)
            back_ref[2 * m + j] = jnp.where(sub < 4, a, b)


def halo_rows(sub, prev_ref, next_ref, p, j):
    a, b = prev_ref[2 * (p // 2) + j], next_ref[2 * (p // 2) + j]
    if p % 2 == 0:
        return jnp.where(sub < 4, b, a)
    return pltpu.roll(jnp.where(sub < 4, a, b), 4, 0)


def cols_kernel(own_ref, prev_ref, next_ref, zp_ref, zn_ref, m_ref):
    sub, lane = iota(0), iota(1)
    from_prev = lanes_of(lane, (0, 1, 2, 10, 11))
    from_next = lanes_of(lane, (7, 8, 9, 16, 17))
    for i in range(NT):
        a = pltpu.roll(prev_ref[i], 128 - 4 * LW, 1)
        b = pltpu.roll(next_ref[i], 4 * LW, 1)
        m_ref[i] = jnp.where(from_prev, a, jnp.where(from_next, b, own_ref[i]))
    acc = jnp.zeros((8, 128), jnp.float32)
    for p in range(NP):
        acc = strip_of(lane, acc, p, halo_rows(sub, zp_ref, zn_ref, p, 0), halo_rows(sub, zp_ref, zn_ref, p, 1))
    m_ref[NT] = acc


def main_kernel(
    sizes, f_ref, l_ref, bp_ref, bn_ref, zp_ref, zn_ref, mp_ref, mn_ref,
    out_hbm, sum_ref,
    ua, ub, qa, qb, v1, v2, wt, at, il, g1, g2, out_ref, sems,
):
    n_tm, n_row, n_col = sizes
    sub, lane = iota(0), iota(1)
    first_t = lax.axis_index("tm") == 0
    last_t = lax.axis_index("tm") == n_tm - 1
    one, zero = jnp.float32(1.0), jnp.float32(0.0)
    last_r = jnp.where(lax.axis_index("row") == n_row - 1, zero, one)
    first_r = jnp.where(lax.axis_index("row") == 0, zero, one)
    last_c = jnp.where(lax.axis_index("col") == n_col - 1, zero, one)
    first_c = jnp.where(lax.axis_index("col") == 0, zero, one)
    ones = jnp.ones((8, 128), jnp.float32)
    row_mask = {NT - 1: jnp.where(sub == 7, ones * last_r, ones), NT: jnp.where(sub == 7, ones * first_r, ones)}
    col_mask = {1: jnp.where(lane == 127, ones * last_c, ones), 2: jnp.where(lane == 127, ones * first_c, ones)}

    def prim(lam, noisy):
        scaled = TAU * lam
        return 1.0 / (1.0 + scaled), scaled * noisy

    def fill_noisy(src, at0, dst):
        for i in range(NT):
            for j in range(2):
                put(ua, dst, i, j, tile(src, at0, i, j))

    def fill_lam(src, at0, dst):
        for i in range(NT):
            for j in range(2):
                w, a = prim(tile(src, at0, i, j), tile(ua, dst + 1, i, j))
                put(wt, dst, i, j, w)
                put(at, dst, i, j, a)

    def own(t, c):
        fill_noisy(f_ref, t, t + 3)
        for i in range(NT):
            for j in range(2):
                lam = tile(l_ref, t, i, j)
                w, a = prim(lam, tile(f_ref, t, i, j))
                put(wt, t + 2, i, j, w)
                put(at, t + 2, i, j, a)
                put(il, t, i, j, 0.5 / lam)
        return c

    lax.fori_loop(0, FR, own, 0)

    def face(k, c):
        fill_noisy(bp_ref, k, k)
        fill_noisy(bn_ref, k, k + 7)
        return c

    lax.fori_loop(0, 3, face, 0)

    def face_lam(k, c):
        fill_lam(bp_ref, 3 + k, k)
        fill_lam(bn_ref, 3 + k, 6 + k)
        return c

    lax.fori_loop(0, 2, face_lam, 0)
    for p in range(NP):
        for j in range(2):
            z = halo_rows(sub, zp_ref, zn_ref, p, j)
            if p < NF:
                put(ua, p, NT, j, z)
            else:
                w, a = prim(z, tile(ua, p - NF + 1, NT, j))
                put(wt, p - NF, NT, j, w)
                put(at, p - NF, NT, j, a)

    from_left = lane % LW < 3
    beside = (lane < 3) | (lane >= 125)

    def side(i, c):
        rows = pl.ds(pl.multiple_of(i * 8, 8), 8)
        strips = jnp.where(from_left, mp_ref[i], mn_ref[i])
        noisy = []
        for p in range(NP):
            x = jnp.where(beside, pltpu.roll(strips, (125 - LW * p) % 128, 1), 0.0)
            if p < NF:
                ua[p, rows, 256:384] = x
                noisy.append(x)
            else:
                w, a = prim(x, noisy[p - NF + 1])
                wt[p - NF, rows, 256:384] = w
                at[p - NF, rows, 256:384] = a
        return c

    lax.fori_loop(0, NTE, side, 0)

    def dual_step(step, u, qi, qo, tt, gi, go, acc):
        inside = acc is not None
        keep = jnp.where(((tt == 6) & last_t) | ((tt == 2) & first_t), zero, one)
        here = [tile(u, tt, 0, j) for j in range(3)]
        start = here
        for i in range(NTE):
            after = start if i == NT else [tile(u, tt, i + 1, j) for j in range(3)]
            turned = [pltpu.roll(here[j], 127, 1) for j in range(3)]
            for j in range(3):
                x = here[j]
                d0 = (tile(u, tt + 1, i, j) - x) * keep
                d1 = pltpu.roll(jnp.where(sub == 0, after[j], x), 7, 0) - x
                if i in row_mask:
                    d1 = d1 * row_mask[i]
                d2 = jnp.where(lane == 127, turned[(j + 1) % 3], turned[j]) - x
                if j in col_mask:
                    d2 = d2 * col_mask[j]
                d = (d0, d1, d2)
                if inside and i < NT and j < 2:
                    gu = d
                    t = tt - 3
                    if step > 0:
                        gu = tuple(0.5 * (d[k] + tile(gi, 4 * k + t, i, j)) for k in range(3))
                    if step < 2:
                        for k in range(3):
                            put(go, 4 * k + t, i, j, gu[k])
                    acc[j] = acc[j] + jnp.sqrt(gu[0] * gu[0] + gu[1] * gu[1] + gu[2] * gu[2])
                m = d if step == 0 else tuple(d[k] + tile(qi, NF * k + tt, i, j) for k in range(3))
                n2 = (m[0] * m[0] + m[1] * m[1] + m[2] * m[2]) * (SIG * SIG)
                s = jnp.minimum(1.0, lax.rsqrt(n2))
                for k in range(3):
                    put(qo, NF * k + tt, i, j, m[k] * s)
            here = after

    def primal_step(step, u, q, vi, vo, uo, tt, acc):
        inside = acc is not None
        nj = 3 if step < 2 else 2
        before = [tile(q, NF + tt, NT, j) for j in range(nj)]
        for i in range(NTE if step < 2 else NT):
            rows = [tile(q, NF + tt, i, j) for j in range(nj)]
            cols = [tile(q, 2 * NF + tt, i, j) for j in range(3)]
            turned = [pltpu.roll(cols[j], 1, 1) for j in range(3)]
            for j in range(nj):
                d = tile(q, tt, i, j) - tile(q, tt - 1, i, j)
                d = d + (rows[j] - pltpu.roll(jnp.where(sub == 7, before[j], rows[j]), 1, 0))
                d = d + (cols[j] - jnp.where(lane == 0, turned[j - 1], turned[j]))
                old = tile(u, tt, i, j) if step == 0 else tile(vi, tt, i, j)
                new = (old + (TAU * SIG) * d + tile(at, tt - 1, i, j)) * tile(wt, tt - 1, i, j)
                if step < 2:
                    put(vo, tt, i, j, new)
                    put(uo, tt, i, j, 2.0 * new - old)
                else:
                    put(out_ref, tt - 3, i, j, new)
                if inside and i < NT and j < 2:
                    t = tt - 3
                    e = SIG * d
                    noisy = tile(f_ref, t, i, j)
                    term = e * (e * tile(il, t, i, j) + noisy)
                    if step > 0:
                        r = old - noisy
                        term = term + (0.5 * tile(l_ref, t, i, j)) * (r * r)
                    acc[j] = acc[j] + term
            before = rows

    def leave(t):
        return pltpu.make_async_copy(out_ref.at[t], out_hbm.at[t], sems.at[t])

    def run(step, u, uo, qi, qo, vi, vo, gi, go):
        lo, hi = step, 8 - step

        def dual_out(k, c):
            dual_step(step, u, qi, qo, jnp.where(k < 3, k, k + 4), gi, go, None)
            return c

        def dual_in(tt, c):
            acc = list(c)
            dual_step(step, u, qi, qo, tt, gi, go, acc)
            return tuple(acc)

        def primal_out(k, c):
            primal_step(step, u, qo, vi, vo, uo, jnp.where(k < 3, k, k + 4), None)
            return c

        def primal_in(tt, c):
            acc = list(c)
            primal_step(step, u, qo, vi, vo, uo, tt, acc)
            if step == 2:
                leave(tt - 3).start()
            return tuple(acc)

        blank = jnp.zeros((8, 128), jnp.float32)
        lax.fori_loop(lo, hi - 3, dual_out, 0)
        acc = lax.fori_loop(3, 7, dual_in, (blank, blank))
        if step < 2:
            lax.fori_loop(lo + 1, hi - 3, primal_out, 0)
        acc = lax.fori_loop(3, 7, primal_in, acc)
        return acc[0] + acc[1]

    s0 = run(0, ua, ub, qb, qa, None, v1, None, g1)
    s1 = run(1, ub, ua, qa, qb, v1, v2, g1, g2)
    s2 = run(2, ua, None, qb, qa, v2, None, g2, None)
    total = [jnp.sum(s) for s in (s0, s1, s2)]
    col = lax.broadcasted_iota(jnp.int32, sum_ref.shape, 1)
    sum_ref[...] = jnp.where(col == 0, total[0], jnp.where(col == 1, total[1], jnp.where(col == 2, total[2], 0.0)))
    for t in range(FR):
        leave(t).wait()


VMEM = pl.BlockSpec(memory_space=pltpu.VMEM)
HBM = pl.BlockSpec(memory_space=pltpu.HBM)


def call(kernel, outs, *args, flops, scratch=(), limit=8 << 20, ins=None, places=None):
    return pl.pallas_call(
        kernel,
        out_shape=outs,
        in_specs=ins or [VMEM] * len(args),
        out_specs=places or jax.tree.map(lambda _: VMEM, outs),
        scratch_shapes=scratch,
        cost_estimate=pl.CostEstimate(flops=flops, bytes_accessed=1 << 20, transcendentals=0),
        compiler_params=pltpu.CompilerParams(vmem_limit_bytes=limit),
    )(*args)


def f32(*shape):
    return jax.ShapeDtypeStruct(shape, jnp.float32)


def both_ways(later, earlier, axis, ring=False):
    n = lax.axis_size(axis)
    pairs = [(i, (i + 1) % n) for i in range(n if ring else n - 1)]
    onward = lax.ppermute(later, axis, pairs)
    back = lax.ppermute(earlier, axis, [(b, a) for a, b in pairs])
    return onward, back


def spread_sum(part, axes):
    n = lax.axis_size(axes)
    rows = jnp.broadcast_to(part, (n, 128))
    return jnp.sum(lax.all_to_all(rows, axes, 0, 0, tiled=True), 0, keepdims=True)


def on_device(noisy, lam):
    n_tm, n_row, n_col = (lax.axis_size(a) for a in ("tm", "row", "col"))
    cells = float(noisy.size * n_tm * n_row * n_col)
    ext = lambda n: pltpu.VMEM((n, NTE * 8, 384), jnp.float32)
    inner = lambda n: pltpu.VMEM((n, 128, 256), jnp.float32)
    strip, z, s_on, s_back, up, down = call(
        pack_kernel,
        (f32(NT, 8, 128), f32(16, 8, 128), f32(NT + 10, 8, 128), f32(NT + 10, 8, 128), f32(5, 128, 256), f32(5, 128, 256)),
        pltpu.with_memory_space_constraint(noisy, pltpu.HBM), pltpu.with_memory_space_constraint(lam, pltpu.HBM),
        flops=1 << 20, ins=[HBM, HBM], limit=8 << 20,
        scratch=[inner(FR), inner(FR), pltpu.SemaphoreType.DMA((2 * FR,))],
    )
    sp, sn = both_ways(s_on, s_back, "tm")
    bp, bn = both_ways(up, down, "tm")
    z_on, z_back = call(rows_kernel, (f32(NP, 8, 128), f32(NP, 8, 128)), z, sp, sn, flops=1 << 20)
    zp, zn = both_ways(z_on, z_back, "row")
    m = call(cols_kernel, f32(NTE, 8, 128), strip, sp, sn, zp, zn, flops=1 << 20)
    mp, mn = both_ways(m, m, "col", ring=True)
    out, part = call(
        functools.partial(main_kernel, (n_tm, n_row, n_col)),
        (f32(4, 128, 256), f32(n_tm * n_col, 128)),
        noisy, lam, bp, bn, zp, zn, mp, mn,
        flops=1 << 26, places=(HBM, VMEM),
        scratch=[ext(NF), ext(NF), ext(3 * NF), ext(3 * NF), ext(NF), ext(NF), ext(NL), ext(NL), inner(4), inner(12), inner(12)]
        + [inner(FR), pltpu.SemaphoreType.DMA((FR,))],
        limit=40 << 20,
    )
    part = jnp.sum(lax.all_to_all(part, ("tm", "col"), 0, 0, tiled=True), 0, keepdims=True)
    gaps = spread_sum(part, "row")[0, :3] / cells
    return out, gaps


def solution(mesh):
    spec = P("tm", "row", "col")
    return jax.shard_map(on_device, mesh=mesh, in_specs=(spec, spec), out_specs=(spec, P()), check_vma=False)
```

```python
import functools

import jax
import jax.numpy as jnp
from jax import lax
from jax.experimental import pallas as pl
from jax.experimental.pallas import tpu as pltpu
from jax.sharding import PartitionSpec as P


SIG = 0.28
TAU = 0.28

FR = 4
NT = 16
NTE = 17
NF = 10
NL = 8
NP = NF + NL
LW = 6


def iota(axis):
    return lax.broadcasted_iota(jnp.int32, (8, 128), axis)


def tile(ref, lead, i, j):
    return ref[lead, i * 8 : (i + 1) * 8, j * 128 : (j + 1) * 128]


def put(ref, lead, i, j, value):
    ref[lead, i * 8 : (i + 1) * 8, j * 128 : (j + 1) * 128] = value


def xtile(ref, lead, i, j):
    return ref[lead, 3 * i + j]


def xput(ref, lead, i, j, value):
    ref[lead, 3 * i + j] = value


def size_of(square):
    return square * lax.rsqrt(jnp.maximum(square, 1e-37))


def strip_of(lane, acc, p, first, last):
    both = pltpu.roll(jnp.where(lane < 64, first, last), (LW * p - 125) % 128, 1)
    return jnp.where((lane >= LW * p) & (lane < LW * p + LW), both, acc)


ZO = NT // 4


def gather4(lane, acc, strip, g, noisy_at, lam_at):
    a = pltpu.roll(strip, (32 * g - LW * noisy_at) % 128, 1)
    b = pltpu.roll(strip, (32 * g + 3 * LW - LW * lam_at) % 128, 1)
    acc = jnp.where((lane >= 32 * g) & (lane < 32 * g + 3 * LW), a, acc)
    return jnp.where((lane >= 32 * g + 3 * LW) & (lane < 32 * g + 5 * LW), b, acc)


def spread4(lane, acc, strips, g, noisy_at, lam_at):
    a = pltpu.roll(strips, (LW * noisy_at - 32 * g) % 128, 1)
    b = pltpu.roll(strips, (LW * lam_at - 32 * g - 3 * LW) % 128, 1)
    acc = jnp.where((lane >= LW * noisy_at) & (lane < LW * noisy_at + 3 * LW), a, acc)
    return jnp.where((lane >= LW * lam_at) & (lane < LW * lam_at + 2 * LW), b, acc)


def pack_kernel(f_hbm, l_hbm, own_ref, z_ref, on_ref, back_ref, up_ref, dn_ref, fv, lv, sems):
    sub, lane = iota(0), iota(1)
    copies = []
    for t in range(FR):
        for k, (src, dst) in enumerate(((f_hbm, fv), (l_hbm, lv))):
            copies.append(pltpu.make_async_copy(src.at[t], dst.at[t], sems.at[2 * t + k]))
            copies[-1].start()
    blank = jnp.zeros((8, 128), jnp.float32)
    strips = [blank] * NT
    for t in range(FR):
        copies[2 * t].wait()
        copies[2 * t + 1].wait()
        for i in range(NT):
            for ref, p in ((fv, t + 3), (lv, t + 12)):
                strips[i] = strip_of(lane, strips[i], p, tile(ref, t, i, 0), tile(ref, t, i, 1))
        for k, ref in ((0, fv), (1, lv)):
            for j in range(2):
                z = jnp.where(sub < 4, tile(ref, t, 0, j), tile(ref, t, NT - 1, j))
                z_ref[2 * (t + 4 * k) + j] = z
                if t >= 1 + k:
                    on_ref[ZO + 2 * (t + 2 * k - 1) + j] = z
                if t < 3 - k:
                    back_ref[ZO + 2 * (t + 3 * k) + j] = z
        if t >= 1:
            up_ref[t - 1] = fv[t]
        if t >= 2:
            up_ref[t + 1] = lv[t]
        if t < 3:
            dn_ref[t] = fv[t]
        if t < 2:
            dn_ref[t + 3] = lv[t]
    for k in range(ZO):
        onward, back = blank, blank
        for g in range(4):
            onward = gather4(lane, onward, strips[4 * k + g], g, 4, 14)
            back = gather4(lane, back, strips[4 * k + g], g, 3, 12)
        on_ref[k] = onward
        back_ref[k] = back
    for i in range(NT):
        own_ref[i] = strips[i]


def rows_kernel(z_ref, prev_ref, next_ref, on_ref, back_ref):
    sub = iota(0)

    def plane(p, j):
        if p < 3:
            return prev_ref[ZO + 2 * p + j]
        if p < 7:
            return z_ref[2 * (p - 3) + j]
        if p < 10:
            return next_ref[ZO + 2 * (p - 7) + j]
        if p < 12:
            return prev_ref[ZO + 2 * (p - 7) + j]
        if p < 16:
            return z_ref[2 * (p - 8) + j]
        return next_ref[ZO + 2 * (p - 13) + j]

    for m in range(NP // 2):
        for j in range(2):
            a, b = plane(2 * m, j), pltpu.roll(plane(2 * m + 1, j), 4, 0)
            on_ref[2 * m + j] = jnp.where(sub < 4, b, a)
            back_ref[2 * m + j] = jnp.where(sub < 4, a, b)


def halo_rows(sub, prev_ref, next_ref, p, j):
    a, b = prev_ref[2 * (p // 2) + j], next_ref[2 * (p // 2) + j]
    if p % 2 == 0:
        return jnp.where(sub < 4, b, a)
    return pltpu.roll(jnp.where(sub < 4, a, b), 4, 0)


def cols_kernel(own_ref, prev_ref, next_ref, zp_ref, zn_ref, m_ref):
    sub, lane = iota(0), iota(1)
    for i in range(NT):
        m = spread4(lane, own_ref[i], prev_ref[i // 4], i % 4, 0, 10)
        m_ref[i] = spread4(lane, m, next_ref[i // 4], i % 4, 7, 16)
    acc = jnp.zeros((8, 128), jnp.float32)
    for p in range(NP):
        acc = strip_of(lane, acc, p, halo_rows(sub, zp_ref, zn_ref, p, 0), halo_rows(sub, zp_ref, zn_ref, p, 1))
    m_ref[NT] = acc


def prim(lam, noisy):
    scaled = TAU * lam
    return 1.0 / (1.0 + scaled), scaled * noisy


def steps_of(sizes, f_ref, l_ref, wt, at, il, out_ref):
    n_tm, n_row, n_col = sizes
    sub, lane = iota(0), iota(1)
    first_t = lax.axis_index("tm") == 0
    last_t = lax.axis_index("tm") == n_tm - 1
    one, zero = jnp.float32(1.0), jnp.float32(0.0)
    last_r = jnp.where(lax.axis_index("row") == n_row - 1, zero, one)
    first_r = jnp.where(lax.axis_index("row") == 0, zero, one)
    last_c = jnp.where(lax.axis_index("col") == n_col - 1, zero, one)
    first_c = jnp.where(lax.axis_index("col") == 0, zero, one)
    ones = jnp.ones((8, 128), jnp.float32)
    row_mask = {NT - 1: jnp.where(sub == 7, ones * last_r, ones), NT: jnp.where(sub == 7, ones * first_r, ones)}
    col_mask = {1: jnp.where(lane == 127, ones * last_c, ones), 2: jnp.where(lane == 127, ones * first_c, ones)}

    def dual_step(step, u, qi, qo, tt, gi, go, acc):
        inside = acc is not None
        keep = jnp.where(((tt == 6) & last_t) | ((tt == 2) & first_t), zero, one)
        here = [xtile(u, tt, 0, j) for j in range(3)]
        start = here
        for i in range(NTE):
            after = start if i == NT else [xtile(u, tt, i + 1, j) for j in range(3)]
            turned = [pltpu.roll(here[j], 127, 1) for j in range(3)]
            for j in range(3):
                x = here[j]
                d0 = (xtile(u, tt + 1, i, j) - x) * keep
                d1 = pltpu.roll(jnp.where(sub == 0, after[j], x), 7, 0) - x
                if i in row_mask:
                    d1 = d1 * row_mask[i]
                d2 = jnp.where(lane == 127, turned[(j + 1) % 3], turned[j]) - x
                if j in col_mask:
                    d2 = d2 * col_mask[j]
                d = (d0, d1, d2)
                if inside and i < NT and j < 2:
                    gu = d
                    t = tt - 3
                    if step > 0:
                        gu = tuple(0.5 * (d[k] + tile(gi, 4 * k + t, i, j)) for k in range(3))
                    if step < 2:
                        for k in range(3):
                            put(go, 4 * k + t, i, j, gu[k])
                    else:
                        acc[j] = acc[j] + size_of(gu[0] * gu[0] + gu[1] * gu[1] + gu[2] * gu[2])
                m = d if step == 0 else tuple(d[k] + xtile(qi, NF * k + tt, i, j) for k in range(3))
                n2 = (m[0] * m[0] + m[1] * m[1] + m[2] * m[2]) * (SIG * SIG)
                s = jnp.minimum(1.0, lax.rsqrt(n2))
                for k in range(3):
                    xput(qo, NF * k + tt, i, j, m[k] * s)
            here = after

    def primal_step(step, u, q, vi, vo, uo, tt, acc):
        inside = acc is not None
        nj = 3 if step < 2 else 2
        before = [xtile(q, NF + tt, NT, j) for j in range(nj)]
        for i in range(NTE if step < 2 else NT):
            rows = [xtile(q, NF + tt, i, j) for j in range(nj)]
            cols = [xtile(q, 2 * NF + tt, i, j) for j in range(3)]
            turned = [pltpu.roll(cols[j], 1, 1) for j in range(3)]
            for j in range(nj):
                d = xtile(q, tt, i, j) - xtile(q, tt - 1, i, j)
                d = d + (rows[j] - pltpu.roll(jnp.where(sub == 7, before[j], rows[j]), 1, 0))
                d = d + (cols[j] - jnp.where(lane == 0, turned[j - 1], turned[j]))
                old = xtile(u, tt, i, j) if step == 0 else xtile(vi, tt, i, j)
                new = (old + (TAU * SIG) * d + xtile(at, tt - 1, i, j)) * xtile(wt, tt - 1, i, j)
                if step < 2:
                    xput(vo, tt, i, j, new)
                    xput(uo, tt, i, j, 2.0 * new - old)
                else:
                    put(out_ref, tt - 3, i, j, new)
                if inside and i < NT and j < 2:
                    t = tt - 3
                    e = SIG * d
                    noisy = tile(f_ref, t, i, j)
                    term = e * (e * tile(il, t, i, j) + noisy)
                    if step > 0:
                        r = old - noisy
                        term = term + (0.5 * tile(l_ref, t, i, j)) * (r * r)
                    acc[j] = acc[j] + term
            before = rows

    return dual_step, primal_step


def prep_kernel(sizes, f_ref, l_ref, zp_ref, zn_ref, mp_ref, mn_ref, ua, ub, qa, v1, wt, at, g1, il, acc_ref):
    sub, lane = iota(0), iota(1)

    def fill_noisy(src, at0, dst):
        for i in range(NT):
            for j in range(2):
                xput(ua, dst, i, j, tile(src, at0, i, j))

    def own(t, c):
        fill_noisy(f_ref, t, t + 3)
        for i in range(NT):
            for j in range(2):
                lam = tile(l_ref, t, i, j)
                w, a = prim(lam, tile(f_ref, t, i, j))
                xput(wt, t + 2, i, j, w)
                xput(at, t + 2, i, j, a)
                put(il, t, i, j, 0.5 / lam)
        return c

    lax.fori_loop(0, FR, own, 0)

    for p in range(NP):
        for j in range(2):
            z = halo_rows(sub, zp_ref, zn_ref, p, j)
            if p < NF:
                xput(ua, p, NT, j, z)
            else:
                w, a = prim(z, xtile(ua, p - NF + 1, NT, j))
                xput(wt, p - NF, NT, j, w)
                xput(at, p - NF, NT, j, a)

    from_left = lane % LW < 3
    beside = (lane < 3) | (lane >= 125)

    def side(i, c):
        strips = jnp.where(from_left, mp_ref[i], mn_ref[i])
        noisy = []
        for p in range(NP):
            x = jnp.where(beside, pltpu.roll(strips, (125 - LW * p) % 128, 1), 0.0)
            if p < NF:
                xput(ua, p, i, 2, x)
                noisy.append(x)
            else:
                w, a = prim(x, noisy[p - NF + 1])
                xput(wt, p - NF, i, 2, w)
                xput(at, p - NF, i, 2, a)
        return c

    lax.fori_loop(0, NTE, side, 0)

    dual_step, primal_step = steps_of(sizes, f_ref, l_ref, wt, at, il, None)

    def dual_in(tt, c):
        dual_step(0, ua, None, qa, tt, None, g1, list(c))
        return c

    def primal_in(tt, c):
        acc = list(c)
        primal_step(0, ua, qa, None, v1, ub, tt, acc)
        return tuple(acc)

    blank = jnp.zeros((8, 128), jnp.float32)
    lax.fori_loop(3, 6, dual_in, (blank, blank))
    acc = lax.fori_loop(4, 6, primal_in, (blank, blank))
    acc_ref[...] = acc[0] + acc[1]


def main_kernel(
    sizes, f_ref, l_ref, bp_ref, bn_ref, il, acc_ref, *refs
):
    (out_hbm, sum_ref, ua, ub, qa, v1, wt, at, g1, qb, v2, g2, out_ref, sems) = refs[7:]
    lane = iota(1)

    def fill_noisy(src, at0, dst):
        for i in range(NT):
            for j in range(2):
                xput(ua, dst, i, j, tile(src, at0, i, j))

    def fill_lam(src, at0, dst):
        for i in range(NT):
            for j in range(2):
                w, a = prim(tile(src, at0, i, j), xtile(ua, dst + 1, i, j))
                xput(wt, dst, i, j, w)
                xput(at, dst, i, j, a)

    def face(k, c):
        fill_noisy(bp_ref, k, k)
        fill_noisy(bn_ref, k, k + 7)
        return c

    lax.fori_loop(0, 3, face, 0)

    def face_lam(k, c):
        fill_lam(bp_ref, 3 + k, k)
        fill_lam(bn_ref, 3 + k, 6 + k)
        return c

    lax.fori_loop(0, 2, face_lam, 0)
    dual_step, primal_step = steps_of(sizes, f_ref, l_ref, wt, at, il, out_ref)

    def leave(t):
        return pltpu.make_async_copy(out_ref.at[t], out_hbm.at[t], sems.at[t])

    def run(step, u, uo, qi, qo, vi, vo, gi, go):
        lo, hi = step, 8 - step

        def dual_out(k, c):
            dual_step(step, u, qi, qo, jnp.where(k < 3, k, k + 4), gi, go, None)
            return c

        def dual_in(tt, c):
            acc = list(c)
            dual_step(step, u, qi, qo, tt, gi, go, acc)
            return tuple(acc)

        def primal_out(k, c):
            primal_step(step, u, qo, vi, vo, uo, jnp.where(k < 3, k, k + 4), None)
            return c

        def primal_in(k, c):
            acc = list(c)
            tt = 3 + 3 * k if step == 0 else k
            primal_step(step, u, qo, vi, vo, uo, tt, acc)
            if step == 2:
                leave(tt - 3).start()
            return tuple(acc)

        blank = jnp.zeros((8, 128), jnp.float32)
        lax.fori_loop(lo, hi - 3, dual_out, 0)
        acc = lax.fori_loop(6 if step == 0 else 3, 7, dual_in, (blank, blank))
        if step < 2:
            lax.fori_loop(lo + 1, hi - 3, primal_out, 0)
        acc = lax.fori_loop(0 if step == 0 else 3, 2 if step == 0 else 7, primal_in, acc)
        return acc[0] + acc[1]

    s0 = acc_ref[...] + run(0, ua, ub, None, qa, None, v1, None, g1)
    s1 = run(1, ub, ua, qa, qb, v1, v2, g1, g2)
    s2 = run(2, ua, None, qb, qa, v2, None, g2, None)

    def variation(t, c):
        acc = list(c)
        for i in range(NT):
            for j in range(2):
                for k, g in enumerate((g1, g2)):
                    x = [tile(g, 4 * n + t, i, j) for n in range(3)]
                    acc[k] = acc[k] + size_of(x[0] * x[0] + x[1] * x[1] + x[2] * x[2])
        return tuple(acc)

    s0, s1 = lax.fori_loop(0, FR, variation, (s0, s1))
    total = [jnp.sum(s) for s in (s0, s1, s2)]
    col = lax.broadcasted_iota(jnp.int32, sum_ref.shape, 1)
    sum_ref[...] = jnp.where(col == 0, total[0], jnp.where(col == 1, total[1], jnp.where(col == 2, total[2], 0.0)))
    for t in range(FR):
        leave(t).wait()


VMEM = pl.BlockSpec(memory_space=pltpu.VMEM)
HBM = pl.BlockSpec(memory_space=pltpu.HBM)


def call(kernel, outs, *args, flops, scratch=(), limit=8 << 20, ins=None, places=None, aliases={}):
    return pl.pallas_call(
        kernel,
        out_shape=outs,
        in_specs=ins or [VMEM] * len(args),
        out_specs=places or jax.tree.map(lambda _: VMEM, outs),
        scratch_shapes=scratch,
        cost_estimate=pl.CostEstimate(flops=flops, bytes_accessed=1 << 20, transcendentals=0),
        compiler_params=pltpu.CompilerParams(vmem_limit_bytes=limit),
        input_output_aliases=aliases,
    )(*args)


def f32(*shape):
    return jax.ShapeDtypeStruct(shape, jnp.float32)


def both_ways(later, earlier, axis, ring=False):
    n = lax.axis_size(axis)
    pairs = [(i, (i + 1) % n) for i in range(n if ring else n - 1)]
    onward = lax.ppermute(later, axis, pairs)
    back = lax.ppermute(earlier, axis, [(b, a) for a, b in pairs])
    return onward, back


def spread_sum(part, axes):
    n = lax.axis_size(axes)
    rows = jnp.broadcast_to(part, (n, 128))
    return jnp.sum(lax.all_to_all(rows, axes, 0, 0, tiled=True), 0, keepdims=True)


def on_device(noisy, lam):
    n_tm, n_row, n_col = (lax.axis_size(a) for a in ("tm", "row", "col"))
    cells = float(noisy.size * n_tm * n_row * n_col)
    ext = lambda n: pltpu.VMEM((n, 3 * NTE + 1, 8, 128), jnp.float32)
    exto = lambda n: f32(n, 3 * NTE + 1, 8, 128)
    inner = lambda n: pltpu.VMEM((n, 128, 256), jnp.float32)
    strip, z, s_on, s_back, up, down, fv, lv = call(
        pack_kernel,
        (f32(NT, 8, 128), f32(16, 8, 128), f32(ZO + 10, 8, 128), f32(ZO + 10, 8, 128), f32(5, 128, 256), f32(5, 128, 256), f32(FR, 128, 256), f32(FR, 128, 256)),
        pltpu.with_memory_space_constraint(noisy, pltpu.HBM), pltpu.with_memory_space_constraint(lam, pltpu.HBM),
        flops=1 << 20, ins=[HBM, HBM], limit=8 << 20,
        scratch=[pltpu.SemaphoreType.DMA((2 * FR,))],
    )
    sp, sn = both_ways(s_on, s_back, "tm")
    bp, bn = both_ways(up, down, "tm")
    z_on, z_back = call(rows_kernel, (f32(NP, 8, 128), f32(NP, 8, 128)), z, sp, sn, flops=1 << 20)
    zp, zn = both_ways(z_on, z_back, "row")
    m = call(cols_kernel, f32(NTE, 8, 128), strip, sp, sn, zp, zn, flops=1 << 20)
    mp, mn = both_ways(m, m, "col", ring=True)
    sizes = (n_tm, n_row, n_col)
    *state, il, acc = call(
        functools.partial(prep_kernel, sizes),
        (exto(NF), exto(NF), exto(3 * NF), exto(NF), exto(NL), exto(NL), f32(12, 128, 256), f32(FR, 128, 256), f32(8, 128)),
        fv, lv, zp, zn, mp, mn,
        flops=1 << 24, limit=4 << 20,
    )
    out, part, *_ = call(
        functools.partial(main_kernel, sizes),
        (f32(4, 128, 256), f32(n_tm * n_col, 128), *(f32(*a.shape) for a in state)),
        fv, lv, bp, bn, il, acc, *state,
        flops=1 << 26, places=(HBM,) + (VMEM,) * 8,
        scratch=[ext(3 * NF), ext(NF), inner(12), inner(FR), pltpu.SemaphoreType.DMA((FR,))],
        aliases={6 + k: 2 + k for k in range(7)},
        limit=16 << 20,
    )
    part = jnp.sum(lax.all_to_all(part, ("tm", "col"), 0, 0, tiled=True), 0, keepdims=True)
    gaps = spread_sum(part, "row")[0, :3] / cells
    return out, gaps


def solution(mesh):
    spec = P("tm", "row", "col")
    return jax.shard_map(on_device, mesh=mesh, in_specs=(spec, spec), out_specs=(spec, P()), check_vma=False)
```

```python
import functools

import jax
import jax.numpy as jnp
from jax import lax
from jax.experimental import pallas as pl
from jax.experimental.pallas import tpu as pltpu
from jax.sharding import PartitionSpec as P


SIG = 0.28
TAU = 0.28

FR = 4
NT = 16
NTE = 17
NF = 10
NL = 8
NP = NF + NL
LW = 6


def iota(axis):
    return lax.broadcasted_iota(jnp.int32, (8, 128), axis)


def tile(ref, lead, i, j):
    return ref[lead, i * 8 : (i + 1) * 8, j * 128 : (j + 1) * 128]


def put(ref, lead, i, j, value):
    ref[lead, i * 8 : (i + 1) * 8, j * 128 : (j + 1) * 128] = value


def xtile(ref, lead, i, j):
    return ref[lead, 3 * i + j]


def xput(ref, lead, i, j, value):
    ref[lead, 3 * i + j] = value


def size_of(square):
    return square * lax.rsqrt(jnp.maximum(square, 1e-37))


def strip_of(lane, acc, p, first, last):
    both = pltpu.roll(jnp.where(lane < 64, first, last), (LW * p - 125) % 128, 1)
    return jnp.where((lane >= LW * p) & (lane < LW * p + LW), both, acc)


ZO = NT // 4


def gather4(lane, acc, strip, g, noisy_at, lam_at):
    a = pltpu.roll(strip, (32 * g - LW * noisy_at) % 128, 1)
    b = pltpu.roll(strip, (32 * g + 3 * LW - LW * lam_at) % 128, 1)
    acc = jnp.where((lane >= 32 * g) & (lane < 32 * g + 3 * LW), a, acc)
    return jnp.where((lane >= 32 * g + 3 * LW) & (lane < 32 * g + 5 * LW), b, acc)


def spread4(lane, acc, strips, g, noisy_at, lam_at):
    a = pltpu.roll(strips, (LW * noisy_at - 32 * g) % 128, 1)
    b = pltpu.roll(strips, (LW * lam_at - 32 * g - 3 * LW) % 128, 1)
    acc = jnp.where((lane >= LW * noisy_at) & (lane < LW * noisy_at + 3 * LW), a, acc)
    return jnp.where((lane >= LW * lam_at) & (lane < LW * lam_at + 2 * LW), b, acc)


def pack_kernel(f_hbm, l_hbm, own_ref, z_ref, on_ref, back_ref, up_ref, dn_ref, fv, lv, sems):
    sub, lane = iota(0), iota(1)
    copies = []
    for t in range(FR):
        for k, (src, dst) in enumerate(((f_hbm, fv), (l_hbm, lv))):
            copies.append(pltpu.make_async_copy(src.at[t], dst.at[t], sems.at[2 * t + k]))
            copies[-1].start()
    blank = jnp.zeros((8, 128), jnp.float32)
    strips = [blank] * NT
    for t in range(FR):
        copies[2 * t].wait()
        copies[2 * t + 1].wait()
        for i in range(NT):
            for ref, p in ((fv, t + 3), (lv, t + 12)):
                strips[i] = strip_of(lane, strips[i], p, tile(ref, t, i, 0), tile(ref, t, i, 1))
        for k, ref in ((0, fv), (1, lv)):
            for j in range(2):
                z = jnp.where(sub < 4, tile(ref, t, 0, j), tile(ref, t, NT - 1, j))
                z_ref[2 * (t + 4 * k) + j] = z
                if t >= 1 + k:
                    on_ref[ZO + 2 * (t + 2 * k - 1) + j] = z
                if t < 3 - k:
                    back_ref[ZO + 2 * (t + 3 * k) + j] = z
        if t >= 1:
            up_ref[t - 1] = fv[t]
        if t >= 2:
            up_ref[t + 1] = lv[t]
        if t < 3:
            dn_ref[t] = fv[t]
        if t < 2:
            dn_ref[t + 3] = lv[t]
    for k in range(ZO):
        onward, back = blank, blank
        for g in range(4):
            onward = gather4(lane, onward, strips[4 * k + g], g, 4, 14)
            back = gather4(lane, back, strips[4 * k + g], g, 3, 12)
        on_ref[k] = onward
        back_ref[k] = back
    for i in range(NT):
        own_ref[i] = strips[i]


def rows_kernel(z_ref, prev_ref, next_ref, on_ref, back_ref):
    sub = iota(0)

    def plane(p, j):
        if p < 3:
            return prev_ref[ZO + 2 * p + j]
        if p < 7:
            return z_ref[2 * (p - 3) + j]
        if p < 10:
            return next_ref[ZO + 2 * (p - 7) + j]
        if p < 12:
            return prev_ref[ZO + 2 * (p - 7) + j]
        if p < 16:
            return z_ref[2 * (p - 8) + j]
        return next_ref[ZO + 2 * (p - 13) + j]

    for m in range(NP // 2):
        for j in range(2):
            a, b = plane(2 * m, j), pltpu.roll(plane(2 * m + 1, j), 4, 0)
            on_ref[2 * m + j] = jnp.where(sub < 4, b, a)
            back_ref[2 * m + j] = jnp.where(sub < 4, a, b)


def halo_rows(sub, prev_ref, next_ref, p, j):
    a, b = prev_ref[2 * (p // 2) + j], next_ref[2 * (p // 2) + j]
    if p % 2 == 0:
        return jnp.where(sub < 4, b, a)
    return pltpu.roll(jnp.where(sub < 4, a, b), 4, 0)


def cols_kernel(own_ref, prev_ref, next_ref, zp_ref, zn_ref, m_ref):
    sub, lane = iota(0), iota(1)
    for i in range(NT):
        m = spread4(lane, own_ref[i], prev_ref[i // 4], i % 4, 0, 10)
        m_ref[i] = spread4(lane, m, next_ref[i // 4], i % 4, 7, 16)
    acc = jnp.zeros((8, 128), jnp.float32)
    for p in range(NP):
        acc = strip_of(lane, acc, p, halo_rows(sub, zp_ref, zn_ref, p, 0), halo_rows(sub, zp_ref, zn_ref, p, 1))
    m_ref[NT] = acc


def prim(lam, noisy):
    scaled = TAU * lam
    return 1.0 / (1.0 + scaled), scaled * noisy


def steps_of(sizes, f_ref, l_ref, wt, at, il, out_ref):
    n_tm, n_row, n_col = sizes
    sub, lane = iota(0), iota(1)
    first_t = lax.axis_index("tm") == 0
    last_t = lax.axis_index("tm") == n_tm - 1
    one, zero = jnp.float32(1.0), jnp.float32(0.0)
    last_r = jnp.where(lax.axis_index("row") == n_row - 1, zero, one)
    first_r = jnp.where(lax.axis_index("row") == 0, zero, one)
    last_c = jnp.where(lax.axis_index("col") == n_col - 1, zero, one)
    first_c = jnp.where(lax.axis_index("col") == 0, zero, one)
    ones = jnp.ones((8, 128), jnp.float32)
    row_mask = {NT - 1: jnp.where(sub == 7, ones * last_r, ones), NT: jnp.where(sub == 7, ones * first_r, ones)}
    col_mask = {1: jnp.where(lane == 127, ones * last_c, ones), 2: jnp.where(lane == 127, ones * first_c, ones)}

    def dual_step(step, u, qi, qo, tt, gi, go, acc, js=(0, 1, 2), rows=NTE, kept=(0, 1, 2)):
        inside = acc is not None
        keep = jnp.where(((tt == 6) & last_t) | ((tt == 2) & first_t), zero, one)
        near = sorted({j for j in js} | {(j + 1) % 3 for j in js})
        here = {j: xtile(u, tt, 0, j) for j in near}
        start = here
        for i in range(rows):
            after = start if i == NT else {j: xtile(u, tt, i + 1, j) for j in near}
            turned = {j: pltpu.roll(here[j], 127, 1) for j in near}
            for j in js:
                x = here[j]
                d0 = (xtile(u, tt + 1, i, j) - x) * keep
                d1 = pltpu.roll(jnp.where(sub == 0, after[j], x), 7, 0) - x
                if i in row_mask:
                    d1 = d1 * row_mask[i]
                d2 = jnp.where(lane == 127, turned[(j + 1) % 3], turned[j]) - x
                if j in col_mask:
                    d2 = d2 * col_mask[j]
                d = (d0, d1, d2)
                if inside and i < NT and j < 2:
                    gu = d
                    t = tt - 3
                    if step > 0:
                        gu = tuple(0.5 * (d[k] + tile(gi, 4 * k + t, i, j)) for k in range(3))
                    if step < 2:
                        for k in range(3):
                            put(go, 4 * k + t, i, j, gu[k])
                    else:
                        acc[j] = acc[j] + size_of(gu[0] * gu[0] + gu[1] * gu[1] + gu[2] * gu[2])
                m = d if step == 0 else tuple(d[k] + xtile(qi, NF * k + tt, i, j) for k in range(3))
                n2 = (m[0] * m[0] + m[1] * m[1] + m[2] * m[2]) * (SIG * SIG)
                s = jnp.minimum(1.0, lax.rsqrt(n2))
                for k in kept:
                    xput(qo, NF * k + tt, i, j, m[k] * s)
            here = after

    def primal_step(step, u, q, vi, vo, uo, tt, acc):
        inside = acc is not None
        nj = 3 if step < 2 else 2
        before = [xtile(q, NF + tt, NT, j) for j in range(nj)]
        for i in range(NTE if step < 2 else NT):
            rows = [xtile(q, NF + tt, i, j) for j in range(nj)]
            cols = [xtile(q, 2 * NF + tt, i, j) for j in range(3)]
            turned = [pltpu.roll(cols[j], 1, 1) for j in range(3)]
            for j in range(nj):
                d = xtile(q, tt, i, j) - xtile(q, tt - 1, i, j)
                d = d + (rows[j] - pltpu.roll(jnp.where(sub == 7, before[j], rows[j]), 1, 0))
                d = d + (cols[j] - jnp.where(lane == 0, turned[j - 1], turned[j]))
                old = xtile(u, tt, i, j) if step == 0 else xtile(vi, tt, i, j)
                new = (old + (TAU * SIG) * d + xtile(at, tt - 1, i, j)) * xtile(wt, tt - 1, i, j)
                if step < 2:
                    xput(vo, tt, i, j, new)
                    xput(uo, tt, i, j, 2.0 * new - old)
                else:
                    put(out_ref, tt - 3, i, j, new)
                if inside and i < NT and j < 2:
                    t = tt - 3
                    e = SIG * d
                    noisy = tile(f_ref, t, i, j)
                    term = e * (e * tile(il, t, i, j) + noisy)
                    if step > 0:
                        r = old - noisy
                        term = term + (0.5 * tile(l_ref, t, i, j)) * (r * r)
                    acc[j] = acc[j] + term
            before = rows

    return dual_step, primal_step


def fill_kernel(sizes, f_ref, l_ref, zp_ref, zn_ref, ua, qa, wt, at, g1, il):
    sub = iota(0)

    def fill_noisy(src, at0, dst):
        for i in range(NT):
            for j in range(2):
                xput(ua, dst, i, j, tile(src, at0, i, j))

    def own(t, c):
        fill_noisy(f_ref, t, t + 3)
        for i in range(NT):
            for j in range(2):
                lam = tile(l_ref, t, i, j)
                w, a = prim(lam, tile(f_ref, t, i, j))
                xput(wt, t + 2, i, j, w)
                xput(at, t + 2, i, j, a)
                put(il, t, i, j, 0.5 / lam)
        return c

    lax.fori_loop(0, FR, own, 0)

    for p in range(NP):
        for j in range(2):
            z = halo_rows(sub, zp_ref, zn_ref, p, j)
            if p < NF:
                xput(ua, p, NT, j, z)
            else:
                w, a = prim(z, xtile(ua, p - NF + 1, NT, j))
                xput(wt, p - NF, NT, j, w)
                xput(at, p - NF, NT, j, a)

    dual_step, _ = steps_of(sizes, f_ref, l_ref, wt, at, il, None)

    def dual_in(tt, c):
        dual_step(0, ua, None, qa, tt, None, g1, [None] * 2, js=(0,))
        return c

    lax.fori_loop(3, 6, dual_in, 0)


def prep_kernel(sizes, f_ref, l_ref, mp_ref, mn_ref, il, *refs):
    (ub, v1, acc_ref, ua, qa, wt, at, g1) = refs[5:]
    lane = iota(1)

    from_left = lane % LW < 3
    beside = (lane < 3) | (lane >= 125)

    def side(i, c):
        strips = jnp.where(from_left, mp_ref[i], mn_ref[i])
        noisy = []
        for p in range(NP):
            x = jnp.where(beside, pltpu.roll(strips, (125 - LW * p) % 128, 1), 0.0)
            if p < NF:
                xput(ua, p, i, 2, x)
                noisy.append(x)
            else:
                w, a = prim(x, noisy[p - NF + 1])
                xput(wt, p - NF, i, 2, w)
                xput(at, p - NF, i, 2, a)
        return c

    lax.fori_loop(0, NTE, side, 0)

    dual_step, primal_step = steps_of(sizes, f_ref, l_ref, wt, at, il, None)

    def dual_in(tt, c):
        dual_step(0, ua, None, qa, tt, None, g1, [None] * 2, js=(1, 2))
        return c

    def primal_in(tt, c):
        acc = list(c)
        primal_step(0, ua, qa, None, v1, ub, tt, acc)
        return tuple(acc)

    blank = jnp.zeros((8, 128), jnp.float32)
    lax.fori_loop(3, 6, dual_in, 0)
    acc = lax.fori_loop(4, 6, primal_in, (blank, blank))
    acc_ref[...] = acc[0] + acc[1]


def main_kernel(
    sizes, f_ref, l_ref, bp_ref, bn_ref, il, acc_ref, *refs
):
    (out_hbm, sum_ref, ua, ub, qa, v1, wt, at, g1, qb, v2, g2, out_ref, sems) = refs[7:]
    lane = iota(1)

    def fill_noisy(src, at0, dst):
        for i in range(NT):
            for j in range(2):
                xput(ua, dst, i, j, tile(src, at0, i, j))

    def fill_lam(src, at0, dst):
        for i in range(NT):
            for j in range(2):
                w, a = prim(tile(src, at0, i, j), xtile(ua, dst + 1, i, j))
                xput(wt, dst, i, j, w)
                xput(at, dst, i, j, a)

    def face(k, c):
        fill_noisy(bp_ref, k, k)
        fill_noisy(bn_ref, k, k + 7)
        return c

    lax.fori_loop(0, 3, face, 0)

    def face_lam(k, c):
        fill_lam(bp_ref, 3 + k, k)
        fill_lam(bn_ref, 3 + k, 6 + k)
        return c

    lax.fori_loop(0, 2, face_lam, 0)
    dual_step, primal_step = steps_of(sizes, f_ref, l_ref, wt, at, il, out_ref)

    def leave(t):
        return pltpu.make_async_copy(out_ref.at[t], out_hbm.at[t], sems.at[t])

    def run(step, u, uo, qi, qo, vi, vo, gi, go):
        lo, hi = step, 8 - step

        def dual_out(k, c):
            dual_step(step, u, qi, qo, jnp.where(k < 3, k, k + 4), gi, go, None)
            return c

        def dual_first():
            if step == 2:
                dual_step(step, u, qi, qo, lo, gi, go, None, js=(0, 1), rows=NT, kept=(0,))
            else:
                dual_step(step, u, qi, qo, lo, gi, go, None, kept=(0,))

        def dual_in(tt, c):
            acc = list(c)
            dual_step(step, u, qi, qo, tt, gi, go, acc)
            return tuple(acc)

        def primal_out(k, c):
            primal_step(step, u, qo, vi, vo, uo, jnp.where(k < 3, k, k + 4), None)
            return c

        def primal_in(k, c):
            acc = list(c)
            tt = 3 + 3 * k if step == 0 else k
            primal_step(step, u, qo, vi, vo, uo, tt, acc)
            if step == 2:
                leave(tt - 3).start()
            return tuple(acc)

        blank = jnp.zeros((8, 128), jnp.float32)
        dual_first()
        if step < 2:
            lax.fori_loop(lo + 1, hi - 3, dual_out, 0)
        acc = lax.fori_loop(6 if step == 0 else 3, 7, dual_in, (blank, blank))
        if step < 2:
            lax.fori_loop(lo + 1, hi - 3, primal_out, 0)
        acc = lax.fori_loop(0 if step == 0 else 3, 2 if step == 0 else 7, primal_in, acc)
        return acc[0] + acc[1]

    s0 = acc_ref[...] + run(0, ua, ub, None, qa, None, v1, None, g1)
    s1 = run(1, ub, ua, qa, qb, v1, v2, g1, g2)
    s2 = run(2, ua, None, qb, qa, v2, None, g2, None)

    def variation(t, c):
        acc = list(c)
        for i in range(NT):
            for j in range(2):
                for k, g in enumerate((g1, g2)):
                    x = [tile(g, 4 * n + t, i, j) for n in range(3)]
                    acc[k] = acc[k] + size_of(x[0] * x[0] + x[1] * x[1] + x[2] * x[2])
        return tuple(acc)

    s0, s1 = lax.fori_loop(0, FR, variation, (s0, s1))
    total = [jnp.sum(s) for s in (s0, s1, s2)]
    col = lax.broadcasted_iota(jnp.int32, sum_ref.shape, 1)
    sum_ref[...] = jnp.where(col == 0, total[0], jnp.where(col == 1, total[1], jnp.where(col == 2, total[2], 0.0)))
    for t in range(FR):
        leave(t).wait()


VMEM = pl.BlockSpec(memory_space=pltpu.VMEM)
HBM = pl.BlockSpec(memory_space=pltpu.HBM)


def call(kernel, outs, *args, flops, scratch=(), limit=8 << 20, ins=None, places=None, aliases={}):
    return pl.pallas_call(
        kernel,
        out_shape=outs,
        in_specs=ins or [VMEM] * len(args),
        out_specs=places or jax.tree.map(lambda _: VMEM, outs),
        scratch_shapes=scratch,
        cost_estimate=pl.CostEstimate(flops=flops, bytes_accessed=1 << 20, transcendentals=0),
        compiler_params=pltpu.CompilerParams(vmem_limit_bytes=limit),
        input_output_aliases=aliases,
    )(*args)


def f32(*shape):
    return jax.ShapeDtypeStruct(shape, jnp.float32)


def both_ways(later, earlier, axis, ring=False):
    n = lax.axis_size(axis)
    pairs = [(i, (i + 1) % n) for i in range(n if ring else n - 1)]
    onward = lax.ppermute(later, axis, pairs)
    back = lax.ppermute(earlier, axis, [(b, a) for a, b in pairs])
    return onward, back


def spread_sum(part, axes):
    n = lax.axis_size(axes)
    rows = jnp.broadcast_to(part, (n, 128))
    return jnp.sum(lax.all_to_all(rows, axes, 0, 0, tiled=True), 0, keepdims=True)


def on_device(noisy, lam):
    n_tm, n_row, n_col = (lax.axis_size(a) for a in ("tm", "row", "col"))
    cells = float(noisy.size * n_tm * n_row * n_col)
    ext = lambda n: pltpu.VMEM((n, 3 * NTE + 1, 8, 128), jnp.float32)
    exto = lambda n: f32(n, 3 * NTE + 1, 8, 128)
    inner = lambda n: pltpu.VMEM((n, 128, 256), jnp.float32)
    strip, z, s_on, s_back, up, down, fv, lv = call(
        pack_kernel,
        (f32(NT, 8, 128), f32(16, 8, 128), f32(ZO + 10, 8, 128), f32(ZO + 10, 8, 128), f32(5, 128, 256), f32(5, 128, 256), f32(FR, 128, 256), f32(FR, 128, 256)),
        pltpu.with_memory_space_constraint(noisy, pltpu.HBM), pltpu.with_memory_space_constraint(lam, pltpu.HBM),
        flops=1 << 20, ins=[HBM, HBM], limit=8 << 20,
        scratch=[pltpu.SemaphoreType.DMA((2 * FR,))],
    )
    sp, sn = both_ways(s_on, s_back, "tm")
    bp, bn = both_ways(up, down, "tm")
    z_on, z_back = call(rows_kernel, (f32(NP, 8, 128), f32(NP, 8, 128)), z, sp, sn, flops=1 << 20)
    zp, zn = both_ways(z_on, z_back, "row")
    m = call(cols_kernel, f32(NTE, 8, 128), strip, sp, sn, zp, zn, flops=1 << 20)
    mp, mn = both_ways(m, m, "col", ring=True)
    sizes = (n_tm, n_row, n_col)
    ua, qa, wt, at, g1, il = call(
        functools.partial(fill_kernel, sizes),
        (exto(NF), exto(3 * NF), exto(NL), exto(NL), f32(12, 128, 256), f32(FR, 128, 256)),
        fv, lv, zp, zn,
        flops=1 << 22, limit=4 << 20,
    )
    ub, v1, acc, ua, qa, wt, at, g1 = call(
        functools.partial(prep_kernel, sizes),
        (exto(NF), exto(NF), f32(8, 128), *(f32(*a.shape) for a in (ua, qa, wt, at, g1))),
        fv, lv, mp, mn, il, ua, qa, wt, at, g1,
        flops=1 << 24, limit=4 << 20, aliases={5 + k: 3 + k for k in range(5)},
    )
    state = (ua, ub, qa, v1, wt, at, g1)
    out, part, *_ = call(
        functools.partial(main_kernel, sizes),
        (f32(4, 128, 256), f32(n_tm * n_col, 128), *(f32(*a.shape) for a in state)),
        fv, lv, bp, bn, il, acc, *state,
        flops=1 << 26, places=(HBM,) + (VMEM,) * 8,
        scratch=[ext(3 * NF), ext(NF), inner(12), inner(FR), pltpu.SemaphoreType.DMA((FR,))],
        aliases={6 + k: 2 + k for k in range(7)},
        limit=16 << 20,
    )
    part = jnp.sum(lax.all_to_all(part, ("tm", "col"), 0, 0, tiled=True), 0, keepdims=True)
    gaps = spread_sum(part, "row")[0, :3] / cells
    return out, gaps


def solution(mesh):
    spec = P("tm", "row", "col")
    return jax.shard_map(on_device, mesh=mesh, in_specs=(spec, spec), out_specs=(spec, P()), check_vma=False)
```

```python
import functools

import jax
import jax.numpy as jnp
from jax import lax
from jax.experimental import pallas as pl
from jax.experimental.pallas import tpu as pltpu
from jax.sharding import PartitionSpec as P


SIG = 0.28
TAU = 0.28

FR = 4
NT = 16
NTE = 17
NF = 10
NL = 8
NP = NF + NL
LW = 6


def iota(axis):
    return lax.broadcasted_iota(jnp.int32, (8, 128), axis)


def tile(ref, lead, i, j):
    return ref[lead, i * 8 : (i + 1) * 8, j * 128 : (j + 1) * 128]


def put(ref, lead, i, j, value):
    ref[lead, i * 8 : (i + 1) * 8, j * 128 : (j + 1) * 128] = value


def xtile(ref, lead, i, j):
    return ref[lead, 3 * i + j]


def xput(ref, lead, i, j, value):
    ref[lead, 3 * i + j] = value


def size_of(square):
    return square * lax.rsqrt(jnp.maximum(square, 1.1754944e-38))


def strip_of(lane, acc, p, first, last):
    both = pltpu.roll(jnp.where(lane < 64, first, last), (LW * p - 125) % 128, 1)
    return jnp.where((lane >= LW * p) & (lane < LW * p + LW), both, acc)


ZO = NT // 4


def gather4(lane, acc, strip, g, noisy_at, lam_at):
    a = pltpu.roll(strip, (32 * g - LW * noisy_at) % 128, 1)
    b = pltpu.roll(strip, (32 * g + 3 * LW - LW * lam_at) % 128, 1)
    acc = jnp.where((lane >= 32 * g) & (lane < 32 * g + 3 * LW), a, acc)
    return jnp.where((lane >= 32 * g + 3 * LW) & (lane < 32 * g + 5 * LW), b, acc)


def spread4(lane, acc, strips, g, noisy_at, lam_at):
    a = pltpu.roll(strips, (LW * noisy_at - 32 * g) % 128, 1)
    b = pltpu.roll(strips, (LW * lam_at - 32 * g - 3 * LW) % 128, 1)
    acc = jnp.where((lane >= LW * noisy_at) & (lane < LW * noisy_at + 3 * LW), a, acc)
    return jnp.where((lane >= LW * lam_at) & (lane < LW * lam_at + 2 * LW), b, acc)


def pack_kernel(f_hbm, l_hbm, own_ref, z_ref, on_ref, back_ref, up_ref, dn_ref, fv, lv, sems):
    sub, lane = iota(0), iota(1)
    copies = []
    for t in range(FR):
        for k, (src, dst) in enumerate(((f_hbm, fv), (l_hbm, lv))):
            copies.append(pltpu.make_async_copy(src.at[t], dst.at[t], sems.at[2 * t + k]))
            copies[-1].start()
    blank = jnp.zeros((8, 128), jnp.float32)
    strips = [blank] * NT
    for t in range(FR):
        copies[2 * t].wait()
        copies[2 * t + 1].wait()
        for i in range(NT):
            for ref, p in ((fv, t + 3), (lv, t + 12)):
                strips[i] = strip_of(lane, strips[i], p, tile(ref, t, i, 0), tile(ref, t, i, 1))
        for k, ref in ((0, fv), (1, lv)):
            for j in range(2):
                z = jnp.where(sub < 4, tile(ref, t, 0, j), tile(ref, t, NT - 1, j))
                z_ref[2 * (t + 4 * k) + j] = z
                if t >= 1 + k:
                    on_ref[ZO + 2 * (t + 2 * k - 1) + j] = z
                if t < 3 - k:
                    back_ref[ZO + 2 * (t + 3 * k) + j] = z
        if t >= 1:
            up_ref[t - 1] = fv[t]
        if t >= 2:
            up_ref[t + 1] = lv[t]
        if t < 3:
            dn_ref[t] = fv[t]
        if t < 2:
            dn_ref[t + 3] = lv[t]
    for k in range(ZO):
        onward, back = blank, blank
        for g in range(4):
            onward = gather4(lane, onward, strips[4 * k + g], g, 4, 14)
            back = gather4(lane, back, strips[4 * k + g], g, 3, 12)
        on_ref[k] = onward
        back_ref[k] = back
    for i in range(NT):
        own_ref[i] = strips[i]


def rows_kernel(z_ref, prev_ref, next_ref, on_ref, back_ref):
    sub = iota(0)

    def plane(p, j):
        if p < 3:
            return prev_ref[ZO + 2 * p + j]
        if p < 7:
            return z_ref[2 * (p - 3) + j]
        if p < 10:
            return next_ref[ZO + 2 * (p - 7) + j]
        if p < 12:
            return prev_ref[ZO + 2 * (p - 7) + j]
        if p < 16:
            return z_ref[2 * (p - 8) + j]
        return next_ref[ZO + 2 * (p - 13) + j]

    for m in range(NP // 2):
        for j in range(2):
            a, b = plane(2 * m, j), pltpu.roll(plane(2 * m + 1, j), 4, 0)
            on_ref[2 * m + j] = jnp.where(sub < 4, b, a)
            back_ref[2 * m + j] = jnp.where(sub < 4, a, b)


def halo_rows(sub, prev_ref, next_ref, p, j):
    a, b = prev_ref[2 * (p // 2) + j], next_ref[2 * (p // 2) + j]
    if p % 2 == 0:
        return jnp.where(sub < 4, b, a)
    return pltpu.roll(jnp.where(sub < 4, a, b), 4, 0)


def cols_kernel(own_ref, prev_ref, next_ref, zp_ref, zn_ref, m_ref):
    sub, lane = iota(0), iota(1)
    for i in range(NT):
        m = spread4(lane, own_ref[i], prev_ref[i // 4], i % 4, 0, 10)
        m_ref[i] = spread4(lane, m, next_ref[i // 4], i % 4, 7, 16)
    acc = jnp.zeros((8, 128), jnp.float32)
    for p in range(NP):
        acc = strip_of(lane, acc, p, halo_rows(sub, zp_ref, zn_ref, p, 0), halo_rows(sub, zp_ref, zn_ref, p, 1))
    m_ref[NT] = acc


def prim(lam, noisy):
    scaled = TAU * lam
    return 1.0 / (1.0 + scaled), scaled * noisy


def steps_of(sizes, f_ref, l_ref, wt, at, il, out_ref):
    n_tm, n_row, n_col = sizes
    sub, lane = iota(0), iota(1)
    first_t = lax.axis_index("tm") == 0
    last_t = lax.axis_index("tm") == n_tm - 1
    one, zero = jnp.float32(1.0), jnp.float32(0.0)
    last_r = jnp.where(lax.axis_index("row") == n_row - 1, zero, one)
    first_r = jnp.where(lax.axis_index("row") == 0, zero, one)
    last_c = jnp.where(lax.axis_index("col") == n_col - 1, zero, one)
    first_c = jnp.where(lax.axis_index("col") == 0, zero, one)
    ones = jnp.ones((8, 128), jnp.float32)
    row_mask = {NT - 1: jnp.where(sub == 7, ones * last_r, ones), NT: jnp.where(sub == 7, ones * first_r, ones)}
    col_mask = {1: jnp.where(lane == 127, ones * last_c, ones), 2: jnp.where(lane == 127, ones * first_c, ones)}

    def dual_step(step, u, qi, qo, tt, gi, go, acc, js=(0, 1, 2), rows=NTE, kept=(0, 1, 2)):
        inside = acc is not None
        onward = jnp.where(((tt == 6) & last_t) | ((tt == 2) & first_t), tt, tt + 1)
        near = sorted({j for j in js} | {(j + 1) % 3 for j in js})
        here = {j: xtile(u, tt, 0, j) for j in near}
        start = here
        for i in range(rows):
            after = start if i == NT else {j: xtile(u, tt, i + 1, j) for j in near}
            turned = {j: pltpu.roll(here[j], 127, 1) for j in near}
            for j in js:
                need = kept
                if inside and step == 2:
                    if i == NT and j == 2:
                        continue
                    need = (1,) if i == NT else (2,) if j == 2 else kept
                x = here[j]
                d0 = xtile(u, onward, i, j) - x
                d1 = pltpu.roll(jnp.where(sub == 0, after[j], x), 7, 0) - x
                if i in row_mask:
                    d1 = d1 * row_mask[i]
                d2 = jnp.where(lane == 127, turned[(j + 1) % 3], turned[j]) - x
                if j in col_mask:
                    d2 = d2 * col_mask[j]
                d = (d0, d1, d2)
                if inside and i < NT and j < 2:
                    gu = d
                    t = tt - 3
                    if step > 0:
                        gu = tuple(0.5 * (d[k] + tile(gi, 4 * k + t, i, j)) for k in range(3))
                    if step < 2:
                        for k in range(3):
                            put(go, 4 * k + t, i, j, gu[k])
                    else:
                        acc[j] = acc[j] + size_of(gu[0] * gu[0] + gu[1] * gu[1] + gu[2] * gu[2])
                m = d if step == 0 else tuple(d[k] + xtile(qi, NF * k + tt, i, j) for k in range(3))
                n2 = (m[0] * m[0] + m[1] * m[1] + m[2] * m[2]) * (SIG * SIG)
                s = jnp.minimum(1.0, lax.rsqrt(n2))
                for k in need:
                    xput(qo, NF * k + tt, i, j, m[k] * s)
            here = after

    def primal_step(step, u, q, vi, vo, uo, tt, acc):
        inside = acc is not None
        nj = 3 if step < 2 else 2
        before = [xtile(q, NF + tt, NT, j) for j in range(nj)]
        for i in range(NTE if step < 2 else NT):
            rows = [xtile(q, NF + tt, i, j) for j in range(nj)]
            cols = [xtile(q, 2 * NF + tt, i, j) for j in range(3)]
            turned = [pltpu.roll(cols[j], 1, 1) for j in range(3)]
            for j in range(nj):
                d = xtile(q, tt, i, j) - xtile(q, tt - 1, i, j)
                d = d + (rows[j] - pltpu.roll(jnp.where(sub == 7, before[j], rows[j]), 1, 0))
                d = d + (cols[j] - jnp.where(lane == 0, turned[j - 1], turned[j]))
                old = xtile(u, tt, i, j) if step == 0 else xtile(vi, tt, i, j)
                new = (old + (TAU * SIG) * d + xtile(at, tt - 1, i, j)) * xtile(wt, tt - 1, i, j)
                if step < 2:
                    xput(vo, tt, i, j, new)
                    xput(uo, tt, i, j, 2.0 * new - old)
                else:
                    put(out_ref, tt - 3, i, j, new)
                if inside and i < NT and j < 2:
                    t = tt - 3
                    e = SIG * d
                    noisy = tile(f_ref, t, i, j)
                    term = e * (e * tile(il, t, i, j) + noisy)
                    if step > 0:
                        r = old - noisy
                        term = term + (0.5 * tile(l_ref, t, i, j)) * (r * r)
                    acc[j] = acc[j] + term
            before = rows

    return dual_step, primal_step


def fill_kernel(sizes, f_ref, l_ref, zp_ref, zn_ref, ua, qa, wt, at, g1, il):
    sub = iota(0)

    def fill_noisy(src, at0, dst):
        for i in range(NT):
            for j in range(2):
                xput(ua, dst, i, j, tile(src, at0, i, j))

    def own(t, c):
        fill_noisy(f_ref, t, t + 3)
        for i in range(NT):
            for j in range(2):
                lam = tile(l_ref, t, i, j)
                w, a = prim(lam, tile(f_ref, t, i, j))
                xput(wt, t + 2, i, j, w)
                xput(at, t + 2, i, j, a)
                put(il, t, i, j, 0.5 / lam)
        return c

    lax.fori_loop(0, FR, own, 0)

    for p in range(NP):
        for j in range(2):
            z = halo_rows(sub, zp_ref, zn_ref, p, j)
            if p < NF:
                xput(ua, p, NT, j, z)
            else:
                w, a = prim(z, xtile(ua, p - NF + 1, NT, j))
                xput(wt, p - NF, NT, j, w)
                xput(at, p - NF, NT, j, a)

    dual_step, _ = steps_of(sizes, f_ref, l_ref, wt, at, il, None)

    def dual_in(tt, c):
        dual_step(0, ua, None, qa, tt, None, g1, [None] * 2, js=(0,))
        return c

    lax.fori_loop(3, 6, dual_in, 0)


def prep_kernel(sizes, f_ref, l_ref, mp_ref, mn_ref, il, *refs):
    (ub, v1, acc_ref, ua, qa, wt, at, g1) = refs[5:]
    lane = iota(1)

    from_left = lane % LW < 3
    beside = (lane < 3) | (lane >= 125)

    def side(i, c):
        strips = jnp.where(from_left, mp_ref[i], mn_ref[i])
        noisy = []
        for p in range(NP):
            x = jnp.where(beside, pltpu.roll(strips, (125 - LW * p) % 128, 1), 0.0)
            if p < NF:
                xput(ua, p, i, 2, x)
                noisy.append(x)
            else:
                w, a = prim(x, noisy[p - NF + 1])
                xput(wt, p - NF, i, 2, w)
                xput(at, p - NF, i, 2, a)
        return c

    lax.fori_loop(0, NTE, side, 0)

    dual_step, primal_step = steps_of(sizes, f_ref, l_ref, wt, at, il, None)

    def dual_in(tt, c):
        dual_step(0, ua, None, qa, tt, None, g1, [None] * 2, js=(1, 2))
        return c

    def primal_in(tt, c):
        acc = list(c)
        primal_step(0, ua, qa, None, v1, ub, tt, acc)
        return tuple(acc)

    blank = jnp.zeros((8, 128), jnp.float32)
    lax.fori_loop(3, 6, dual_in, 0)
    acc = lax.fori_loop(4, 6, primal_in, (blank, blank))
    acc_ref[...] = acc[0] + acc[1]


def main_kernel(
    sizes, f_ref, l_ref, bp_ref, bn_ref, il, acc_ref, *refs
):
    (out_hbm, sum_ref, ua, ub, qa, v1, wt, at, g1, qb, v2, g2, out_ref, sems) = refs[7:]
    lane = iota(1)

    def fill_noisy(src, at0, dst):
        for i in range(NT):
            for j in range(2):
                xput(ua, dst, i, j, tile(src, at0, i, j))

    def fill_lam(src, at0, dst):
        for i in range(NT):
            for j in range(2):
                w, a = prim(tile(src, at0, i, j), xtile(ua, dst + 1, i, j))
                xput(wt, dst, i, j, w)
                xput(at, dst, i, j, a)

    def face(k, c):
        fill_noisy(bp_ref, k, k)
        fill_noisy(bn_ref, k, k + 7)
        return c

    lax.fori_loop(0, 3, face, 0)

    def face_lam(k, c):
        fill_lam(bp_ref, 3 + k, k)
        fill_lam(bn_ref, 3 + k, 6 + k)
        return c

    lax.fori_loop(0, 2, face_lam, 0)
    dual_step, primal_step = steps_of(sizes, f_ref, l_ref, wt, at, il, out_ref)

    def leave(t):
        return pltpu.make_async_copy(out_ref.at[t], out_hbm.at[t], sems.at[t])

    def run(step, u, uo, qi, qo, vi, vo, gi, go):
        lo, hi = step, 8 - step

        def dual_out(k, c):
            dual_step(step, u, qi, qo, jnp.where(k < 3, k, k + 4), gi, go, None)
            return c

        def dual_first():
            if step == 2:
                dual_step(step, u, qi, qo, lo, gi, go, None, js=(0, 1), rows=NT, kept=(0,))
            else:
                dual_step(step, u, qi, qo, lo, gi, go, None, kept=(0,))

        def dual_in(tt, c):
            acc = list(c)
            dual_step(step, u, qi, qo, tt, gi, go, acc)
            return tuple(acc)

        def primal_out(k, c):
            primal_step(step, u, qo, vi, vo, uo, jnp.where(k < 3, k, k + 4), None)
            return c

        def primal_in(k, c):
            acc = list(c)
            tt = 3 + 3 * k if step == 0 else k
            primal_step(step, u, qo, vi, vo, uo, tt, acc)
            if step == 2:
                leave(tt - 3).start()
            return tuple(acc)

        blank = jnp.zeros((8, 128), jnp.float32)
        dual_first()
        if step < 2:
            lax.fori_loop(lo + 1, hi - 3, dual_out, 0)
        acc = lax.fori_loop(6 if step == 0 else 3, 7, dual_in, (blank, blank))
        if step < 2:
            lax.fori_loop(lo + 1, hi - 3, primal_out, 0)
        acc = lax.fori_loop(0 if step == 0 else 3, 2 if step == 0 else 7, primal_in, acc)
        return acc[0] + acc[1]

    s0 = acc_ref[...] + run(0, ua, ub, None, qa, None, v1, None, g1)
    s1 = run(1, ub, ua, qa, qb, v1, v2, g1, g2)
    s2 = run(2, ua, None, qb, qa, v2, None, g2, None)

    def variation(t, c):
        acc = list(c)
        for i in range(NT):
            for j in range(2):
                for k, g in enumerate((g1, g2)):
                    x = [tile(g, 4 * n + t, i, j) for n in range(3)]
                    acc[k] = acc[k] + size_of(x[0] * x[0] + x[1] * x[1] + x[2] * x[2])
        return tuple(acc)

    s0, s1 = lax.fori_loop(0, FR, variation, (s0, s1))
    total = [jnp.sum(s) for s in (s0, s1, s2)]
    col = lax.broadcasted_iota(jnp.int32, sum_ref.shape, 1)
    sum_ref[...] = jnp.where(col == 0, total[0], jnp.where(col == 1, total[1], jnp.where(col == 2, total[2], 0.0)))
    for t in range(FR):
        leave(t).wait()


VMEM = pl.BlockSpec(memory_space=pltpu.VMEM)
HBM = pl.BlockSpec(memory_space=pltpu.HBM)


def call(kernel, outs, *args, flops, scratch=(), limit=8 << 20, ins=None, places=None, aliases={}):
    return pl.pallas_call(
        kernel,
        out_shape=outs,
        in_specs=ins or [VMEM] * len(args),
        out_specs=places or jax.tree.map(lambda _: VMEM, outs),
        scratch_shapes=scratch,
        cost_estimate=pl.CostEstimate(flops=flops, bytes_accessed=1 << 20, transcendentals=0),
        compiler_params=pltpu.CompilerParams(vmem_limit_bytes=limit),
        input_output_aliases=aliases,
    )(*args)


def f32(*shape):
    return jax.ShapeDtypeStruct(shape, jnp.float32)


def both_ways(later, earlier, axis, ring=False):
    n = lax.axis_size(axis)
    pairs = [(i, (i + 1) % n) for i in range(n if ring else n - 1)]
    onward = lax.ppermute(later, axis, pairs)
    back = lax.ppermute(earlier, axis, [(b, a) for a, b in pairs])
    return onward, back


def spread_sum(part, axes):
    n = lax.axis_size(axes)
    rows = jnp.broadcast_to(part, (n, 128))
    return jnp.sum(lax.all_to_all(rows, axes, 0, 0, tiled=True), 0, keepdims=True)


def on_device(noisy, lam):
    n_tm, n_row, n_col = (lax.axis_size(a) for a in ("tm", "row", "col"))
    cells = float(noisy.size * n_tm * n_row * n_col)
    ext = lambda n: pltpu.VMEM((n, 3 * NTE + 1, 8, 128), jnp.float32)
    exto = lambda n: f32(n, 3 * NTE + 1, 8, 128)
    inner = lambda n: pltpu.VMEM((n, 128, 256), jnp.float32)
    strip, z, s_on, s_back, up, down, fv, lv = call(
        pack_kernel,
        (f32(NT, 8, 128), f32(16, 8, 128), f32(ZO + 10, 8, 128), f32(ZO + 10, 8, 128), f32(5, 128, 256), f32(5, 128, 256), f32(FR, 128, 256), f32(FR, 128, 256)),
        pltpu.with_memory_space_constraint(noisy, pltpu.HBM), pltpu.with_memory_space_constraint(lam, pltpu.HBM),
        flops=1 << 20, ins=[HBM, HBM], limit=8 << 20,
        scratch=[pltpu.SemaphoreType.DMA((2 * FR,))],
    )
    sp, sn = both_ways(s_on, s_back, "tm")
    bp, bn = both_ways(up, down, "tm")
    z_on, z_back = call(rows_kernel, (f32(NP, 8, 128), f32(NP, 8, 128)), z, sp, sn, flops=1 << 20)
    zp, zn = both_ways(z_on, z_back, "row")
    m = call(cols_kernel, f32(NTE, 8, 128), strip, sp, sn, zp, zn, flops=1 << 20)
    mp, mn = both_ways(m, m, "col", ring=True)
    sizes = (n_tm, n_row, n_col)
    ua, qa, wt, at, g1, il = call(
        functools.partial(fill_kernel, sizes),
        (exto(NF), exto(3 * NF), exto(NL), exto(NL), f32(12, 128, 256), f32(FR, 128, 256)),
        fv, lv, zp, zn,
        flops=1 << 22, limit=4 << 20,
    )
    ub, v1, acc, ua, qa, wt, at, g1 = call(
        functools.partial(prep_kernel, sizes),
        (exto(NF), exto(NF), f32(8, 128), *(f32(*a.shape) for a in (ua, qa, wt, at, g1))),
        fv, lv, mp, mn, il, ua, qa, wt, at, g1,
        flops=1 << 24, limit=4 << 20, aliases={5 + k: 3 + k for k in range(5)},
    )
    state = (ua, ub, qa, v1, wt, at, g1)
    out, part, *_ = call(
        functools.partial(main_kernel, sizes),
        (f32(4, 128, 256), f32(n_tm * n_col, 128), *(f32(*a.shape) for a in state)),
        fv, lv, bp, bn, il, acc, *state,
        flops=1 << 26, places=(HBM,) + (VMEM,) * 8,
        scratch=[ext(3 * NF), ext(NF), inner(12), inner(FR), pltpu.SemaphoreType.DMA((FR,))],
        aliases={6 + k: 2 + k for k in range(7)},
        limit=16 << 20,
    )
    part = jnp.sum(lax.all_to_all(part, ("tm", "col"), 0, 0, tiled=True), 0, keepdims=True)
    gaps = spread_sum(part, "row")[0, :3] / cells
    return out, gaps


def solution(mesh):
    spec = P("tm", "row", "col")
    return jax.shard_map(on_device, mesh=mesh, in_specs=(spec, spec), out_specs=(spec, P()), check_vma=False)
```
